32 devices in a mesh: tile: 8 (over z, y), slab: 4 (over x, core).
Axes of the slice: x: 2, y: 2, z: 4, core: 2. Of those that a mesh axis runs over, the one named last changes fastest.
Arguments:
- snapshots: float32 [64, 61440], P('tile', 'slab'), as said below
- old_basis: float32 [61440, 512], P(('slab', 'tile'))
- sing_values: float32 [512], replicated, may hold values from 2 to 8
Outputs:
- new_basis: bfloat16 [61440, 512], P(('slab', 'tile'))
The draws below stay inside these ranges and needn't reach their ends.
Inputs may be any that keep to these rules, and one draw needn't show every extreme that they name: Each snapshot is a combination of the resident modes plus a residual part whose size differs strongly between snapshots and grows along the cells.
All inputs are finite; a program needn't handle non-finite values.
Results may differ from the reference program's by a relative error of at most 0.001.
Values sent between devices are 32-bit elements; how exact they have to be, the bound alone decides.
No kernel may reach another device: no remote copies, remote signals or barrier semaphores. Data moves between devices by JAX's collectives and lax.ppermute only.
A program may use at most 64 MiB of HBM per device.

```python
import math
import jax
import jax.numpy as jnp
from jax import lax

MODES = 512
SNAPS = 64
CELLS = 61440


def common_basis(key):
    return jax.random.normal(jax.random.fold_in(key, 11), (CELLS, MODES), jnp.float32)


def draw_old_basis(key, part):
    return common_basis(key)


def draw_snapshots(key, part):
    modes_part = common_basis(key)
    mixing = 0.8 * jax.random.normal(jax.random.fold_in(key, 12), (MODES, SNAPS), jnp.float32)
    log_scale = jax.random.uniform(jax.random.fold_in(key, 13), (SNAPS,), jnp.float32, 0.0, jnp.log(10.0))
    position = jnp.arange(CELLS, dtype=jnp.float32) / CELLS
    ramp = 1.0 + 2.0 * position
    noise = jax.random.normal(jax.random.fold_in(key, 14), (SNAPS, CELLS), jnp.float32)
    signal = jnp.dot(mixing.T, modes_part.T, preferred_element_type=jnp.float32)
    return signal + noise * jnp.exp(log_scale)[:, None] * ramp[None, :]


def setup_inputs(seed: int = 0) -> dict:
    splits = jax.random.split(jax.random.key(seed), 4)
    snapshots = draw_snapshots(jax.random.fold_in(splits[3], 71), 0)
    old_basis = draw_old_basis(jax.random.fold_in(splits[3], 71), 0)
    sing_values = jnp.clip(jnp.exp(jax.random.uniform(splits[2], (MODES,), jnp.float32, math.log(2.0), math.log(8.0))), 2.0, 8.0)
    return {"snapshots": snapshots, "old_basis": old_basis, "sing_values": sing_values}


HIGH = lax.Precision.HIGHEST

def tri_solve(lower, rows):
    return lax.linalg.triangular_solve(lower, rows, left_side=True, lower=True)

def chol_rows(rows, factor):
    gram_mat = jnp.dot(rows.astype(jnp.float32), rows.T.astype(jnp.float32), precision=HIGH, preferred_element_type=jnp.float32) * factor
    lower = jnp.linalg.cholesky(gram_mat)
    return (tri_solve(lower, rows), lower)

def rotation_of(coeffs, factor_mat, sing_values):
    upper_block = jnp.diag(sing_values * sing_values) + jnp.dot(coeffs.T.astype(jnp.float32), coeffs.astype(jnp.float32), precision=HIGH, preferred_element_type=jnp.float32)
    lower_block = jnp.dot(factor_mat.T.astype(jnp.float32), coeffs.astype(jnp.float32), precision=HIGH, preferred_element_type=jnp.float32)
    stacked = jnp.concatenate([upper_block, lower_block], axis=0)
    for repeat_index in range(2):
        gram_mat = jnp.dot(stacked.T.astype(jnp.float32), stacked.astype(jnp.float32), precision=HIGH, preferred_element_type=jnp.float32)
        lower = jnp.linalg.cholesky(gram_mat)
        stacked = tri_solve(lower, stacked.T).T
    return stacked

def reference(snapshots, old_basis, sing_values):
    weight_cell = 1.0 / CELLS
    coeffs = jnp.dot(snapshots.astype(jnp.float32), old_basis.astype(jnp.float32), precision=HIGH, preferred_element_type=jnp.float32) * weight_cell
    resid = snapshots - jnp.dot(coeffs.astype(jnp.float32), old_basis.T.astype(jnp.float32), precision=HIGH, preferred_element_type=jnp.float32)
    ortho, lower_one = chol_rows(resid, weight_cell)
    rotation = rotation_of(coeffs, lower_one, sing_values)
    modes = old_basis.shape[1]
    result = jnp.dot(old_basis.astype(jnp.float32), rotation[:modes].astype(jnp.float32), precision=HIGH, preferred_element_type=jnp.float32)
    result = result + jnp.dot(ortho.T.astype(jnp.float32), rotation[modes:].astype(jnp.float32), precision=HIGH, preferred_element_type=jnp.float32)
    return result.astype(jnp.bfloat16)
```

```python
import jax
import jax.numpy as jnp
from jax import lax
from jax.sharding import PartitionSpec as P

HIGH = lax.Precision.HIGH
HIGHEST = lax.Precision.HIGHEST


def mat(left, right, contract, precision):
    return lax.dot_general(
        left, right, (contract, ((), ())), precision=precision, preferred_element_type=jnp.float32
    )


def tri_inverse(lower):
    eye = jnp.eye(lower.shape[0], dtype=jnp.float32)
    return lax.linalg.triangular_solve(lower, eye, left_side=True, lower=True)


def pair_rounds():
    rounds = []
    for name in ("slab", "tile"):
        size = lax.axis_size(name)
        step = 1
        while step < size:
            rounds.append((name, [(i, i ^ step) for i in range(size)]))
            step *= 2
    return rounds


def sum_all(part):
    for name, pairs in pair_rounds():
        part = part + lax.ppermute(part, name, pairs)
    return part


def sum_all_halved(part):
    rounds = pair_rounds()
    half = part.shape[0] // 2
    first = lax.axis_index(rounds[0][0]) % 2 == 0
    top, low = part[:half], part[half:]
    kept = jnp.where(first, top, low) + lax.ppermute(jnp.where(first, low, top), *rounds[0])
    for name, pairs in rounds[1:]:
        kept = kept + lax.ppermute(kept, name, pairs)
    other = lax.ppermute(kept, *rounds[0])
    return jnp.concatenate([jnp.where(first, kept, other), jnp.where(first, other, kept)], axis=0)


def local(snapshots, old_basis, sing_values):
    snap_rows = lax.all_to_all(snapshots, "tile", split_axis=1, concat_axis=0, tiled=True)
    cell_count = old_basis.shape[0] * lax.axis_size("tile") * lax.axis_size("slab")
    weight_cell = 1.0 / cell_count
    coeffs = sum_all_halved(mat(snap_rows, old_basis, ((1,), (0,)), HIGH) * weight_cell)
    resid = snap_rows - mat(coeffs, old_basis, ((1,), (1,)), HIGH)
    gram_res = sum_all(mat(resid, resid, ((1,), (1,)), HIGH) * weight_cell)
    squares = sing_values * sing_values
    mixed = old_basis * squares + mat(snap_rows, coeffs, ((0,), (0,)), HIGH)
    upper = jnp.diag(squares) + mat(coeffs, coeffs, ((0,), (0,)), HIGHEST)
    gram_one = mat(upper, upper, ((1,), (1,)), HIGHEST) + mat(
        coeffs, mat(gram_res, coeffs, ((1,), (0,)), HIGHEST), ((0,), (0,)), HIGHEST
    )
    inv_one = tri_inverse(jnp.linalg.cholesky(gram_one))
    upper_two = mat(inv_one, upper, ((1,), (0,)), HIGHEST)
    coeffs_two = mat(inv_one, coeffs, ((1,), (1,)), HIGHEST)
    gram_two = mat(upper_two, upper_two, ((1,), (1,)), HIGHEST) + mat(
        mat(coeffs_two, gram_res, ((1,), (0,)), HIGHEST), coeffs_two, ((1,), (1,)), HIGHEST
    )
    inv_two = tri_inverse(jnp.linalg.cholesky(gram_two))
    turn = mat(inv_two, inv_one, ((1,), (0,)), HIGHEST)
    return mat(mixed, turn, ((1,), (1,)), HIGH).astype(jnp.bfloat16)


def solution(mesh):
    placed = (P("tile", "slab"), P(("slab", "tile"), None), P())
    return jax.shard_map(
        local, mesh=mesh, in_specs=placed, out_specs=P(("slab", "tile"), None), check_vma=False
    )
```

```python
import jax
import jax.numpy as jnp
from jax import lax
from jax.experimental import pallas as pl
from jax.experimental.pallas import tpu as pltpu
from jax.sharding import PartitionSpec as P

HIGHEST = lax.Precision.HIGHEST
BLOCK = 128


def dot(left, right, contract=((1,), (0,)), precision=HIGHEST):
    return lax.dot_general(
        left, right, (contract, ((), ())), precision=precision, preferred_element_type=jnp.float32
    )


def factor_block(work):
    size = work.shape[0]
    lanes = lax.broadcasted_iota(jnp.int32, (8, size), 1)
    subs = lax.broadcasted_iota(jnp.int32, (8, size), 0)
    full = (8, size)
    for step in range(size // 8):
        base = 8 * step
        inside = (lanes >= base) & (lanes < base + 8)
        row = work[pl.ds(base, 8), :]
        cols = [jnp.broadcast_to(row[:, base + j : base + j + 1], full) for j in range(8)]
        entry = {
            (i, j): jnp.broadcast_to(cols[j][i : i + 1, :], full) for j in range(8) for i in range(j, 8)
        }
        ratio, recip = {}, []
        for j in range(8):
            recip.append(1.0 / entry[j, j])
            for k in range(j + 1, 8):
                ratio[j, k] = entry[k, j] * recip[j]
            for k in range(j + 1, 8):
                for i in range(k, 8):
                    entry[i, k] = entry[i, k] - entry[i, j] * ratio[j, k]
        pivots = entry[0, 0]
        for j in range(1, 8):
            pivots = jnp.where(subs == j, entry[j, j], pivots)
        for k in range(1, 8):
            for j in range(k):
                cols[k] = cols[k] - cols[j] * ratio[j, k]
        row = jnp.where(inside, jnp.where(lanes - base == subs, 1.0, 0.0), row)
        scaled = []
        for j in range(8):
            scaled.append(jnp.broadcast_to(row[j : j + 1, :], full) * recip[j])
            if j < 7:
                row = row - jnp.where(subs > j, cols[j], 0.0) * scaled[j]
        work[pl.ds(base, 8), :] = row * lax.rsqrt(pivots)
        for other in range(step + 1, size // 8):
            below = work[pl.ds(8 * other, 8), :]
            cols = [jnp.broadcast_to(below[:, base + j : base + j + 1], full) for j in range(8)]
            for k in range(1, 8):
                for j in range(k):
                    cols[k] = cols[k] - cols[j] * ratio[j, k]
            terms = [cols[j] * scaled[j] for j in range(8)]
            while len(terms) > 1:
                terms = [a + b for a, b in zip(terms[::2], terms[1::2])]
            work[pl.ds(8 * other, 8), :] = jnp.where(inside, 0.0, below) - terms[0]


def tril(value):
    rows = lax.broadcasted_iota(jnp.int32, value.shape, 0)
    return jnp.where(lax.broadcasted_iota(jnp.int32, value.shape, 1) <= rows, value, 0.0)


def factor_inverse(gram, work):
    size = gram.shape[0]
    count = size // BLOCK

    def step(index, carry):
        start = pl.multiple_of(index * BLOCK, BLOCK)
        here = pl.ds(start, BLOCK)
        work[...] = gram[here, here]
        factor_block(work)
        inverse = tril(work[...])
        gram[here, here] = jnp.eye(BLOCK, dtype=jnp.float32)
        for block in range(count):

            @pl.when(index == block)
            def _():
                low = BLOCK * block
                rest = size - low - BLOCK
                row = dot(inverse, gram[pl.ds(low, BLOCK), :])
                gram[pl.ds(low, BLOCK), :] = row
                if rest:
                    turned = row[:, low + BLOCK :].T
                    gram[pl.ds(low + BLOCK, rest), pl.ds(low, BLOCK)] = jnp.zeros(
                        (rest, BLOCK), jnp.float32
                    )
                    for other in range(0, rest, BLOCK):
                        rows = pl.ds(low + BLOCK + other, BLOCK)
                        gram[rows, :] = gram[rows, :] - dot(turned[other : other + BLOCK], row)

        return carry

    lax.fori_loop(0, count, step, 0)
    gram[...] = tril(gram[...])


def diagonal(value):
    rows = lax.broadcasted_iota(jnp.int32, value.shape, 0)
    cols = lax.broadcasted_iota(jnp.int32, value.shape, 1)
    return rows == cols


def half(value):
    rows = lax.broadcasted_iota(jnp.int32, value.shape, 0)
    cols = lax.broadcasted_iota(jnp.int32, value.shape, 1)
    return jnp.where(rows > cols, value, jnp.where(rows == cols, 0.5 * value, 0.0))


def dot3(left, right, contract=((1,), (0,))):
    left_top = left.astype(jnp.bfloat16)
    right_top = right.astype(jnp.bfloat16)
    left_low = (left - left_top.astype(jnp.float32)).astype(jnp.bfloat16)
    right_low = (right - right_top.astype(jnp.float32)).astype(jnp.bfloat16)
    small = dot(left_low, right_top, contract, None) + dot(left_top, right_low, contract, None)
    return dot(left_top, right_top, contract, None) + small


NT = ((1,), (1,))
STOP = 1e-5
NEAR = 0.2


def rotation_kernel(coeffs_ref, gram_ref, squares_ref, cells_ref, snaps_ref, inv_one, inv_two, upper, work):
    coeffs = coeffs_ref[...]
    modes = coeffs.shape[1]
    squares = squares_ref[...]
    coeffs_turned = coeffs.T
    square = dot(coeffs_turned, coeffs)
    upper[...] = square + jnp.where(diagonal(square), squares, 0.0)
    inv_one[...] = dot(upper[...], upper[...]) + dot(
        coeffs_turned, dot(gram_ref[...], coeffs)
    )
    factor_inverse(inv_one, work)
    stacked = dot(inv_one[...], upper[...])
    part = dot(inv_one[...], coeffs_turned)
    gram_two = dot(stacked, stacked, NT) + dot(dot(part, gram_ref[...]), part, NT)
    inv_two[...] = gram_two
    rest = gram_two - jnp.where(diagonal(gram_two), 1.0, 0.0)
    size = jnp.sum(rest * rest)
    near = size < NEAR

    @pl.when(near)
    def _():
        upper[...] = rest

        def more(carry):
            return (carry[0] >= STOP) & (carry[1] < 16)

        def newton(carry):
            rest = upper[...]
            low = half(rest)
            inv_one[...] = inv_one[...] - dot3(low, inv_one[...])
            mixed = dot3(low, rest)
            rest = dot3(low + mixed, low, NT) - mixed - mixed.T
            upper[...] = rest
            return jnp.sum(rest * rest), carry[1] + 1

        lax.while_loop(more, newton, (size, jnp.int32(0)))
        inv_one[...] = inv_one[...] - dot3(half(upper[...]), inv_one[...])

    @pl.when(jnp.logical_not(near))
    def _():
        factor_inverse(inv_two, work)
        inv_one[...] = dot(inv_two[...], inv_one[...])

    cells_ref[...] = inv_one[...] * squares
    snaps_ref[...] = dot(coeffs, inv_one[...], NT)


def rotation_of(coeffs, gram_res, squares):
    snaps, modes = coeffs.shape
    whole = pltpu.VMEM((modes, modes), jnp.float32)
    spec = pl.BlockSpec(memory_space=pltpu.VMEM)
    return pl.pallas_call(
        rotation_kernel,
        out_shape=(
            jax.ShapeDtypeStruct((modes, modes), jnp.float32),
            jax.ShapeDtypeStruct((snaps, modes), jnp.float32),
        ),
        in_specs=[spec] * 3,
        out_specs=(spec, spec),
        scratch_shapes=[whole, whole, whole, pltpu.VMEM((BLOCK, BLOCK), jnp.float32)],
    )(coeffs, gram_res, squares)


HIGH = lax.Precision.HIGH


def mat(left, right, contract, precision=HIGH):
    return lax.dot_general(
        left, right, (contract, ((), ())), precision=precision, preferred_element_type=jnp.float32
    )


def pair_rounds():
    rounds = []
    for name in ("slab", "tile"):
        size = lax.axis_size(name)
        step = 1
        while step < size:
            rounds.append((name, [(i, i ^ step) for i in range(size)]))
            step *= 2
    return rounds


def sum_all(part):
    for name, pairs in pair_rounds():
        part = part + lax.ppermute(part, name, pairs)
    return part


def sum_all_halved(part):
    rounds = pair_rounds()
    half_rows = part.shape[0] // 2
    first = lax.axis_index(rounds[0][0]) % 2 == 0
    top, low = part[:half_rows], part[half_rows:]
    kept = jnp.where(first, top, low) + lax.ppermute(jnp.where(first, low, top), *rounds[0])
    for name, pairs in rounds[1:]:
        kept = kept + lax.ppermute(kept, name, pairs)
    other = lax.ppermute(kept, *rounds[0])
    return jnp.concatenate([jnp.where(first, kept, other), jnp.where(first, other, kept)], axis=0)


def local(snapshots, old_basis, sing_values):
    snap_rows = lax.all_to_all(snapshots, "tile", split_axis=1, concat_axis=0, tiled=True)
    cell_count = old_basis.shape[0] * lax.axis_size("tile") * lax.axis_size("slab")
    weight_cell = 1.0 / cell_count
    coeffs = sum_all_halved(mat(snap_rows, old_basis, ((1,), (0,))) * weight_cell)
    resid = snap_rows - mat(coeffs, old_basis, ((1,), (1,)))
    gram_res = sum_all(mat(resid, resid, ((1,), (1,))) * weight_cell)
    squares = (sing_values * sing_values)[None, :]
    turn_cells, turn_snaps = rotation_of(coeffs, gram_res, squares)
    result = mat(old_basis, turn_cells, ((1,), (1,))) + mat(snap_rows, turn_snaps, ((0,), (0,)))
    return result.astype(jnp.bfloat16)


def solution(mesh):
    placed = (P("tile", "slab"), P(("slab", "tile"), None), P())
    return jax.shard_map(
        local, mesh=mesh, in_specs=placed, out_specs=P(("slab", "tile"), None), check_vma=False
    )
```

```python
import jax
import jax.numpy as jnp
from jax import lax
from jax.experimental import pallas as pl
from jax.experimental.pallas import tpu as pltpu
from jax.sharding import PartitionSpec as P

HIGHEST = lax.Precision.HIGHEST
BLOCK = 128


def dot(left, right, contract=((1,), (0,)), precision=HIGHEST):
    return lax.dot_general(
        left, right, (contract, ((), ())), precision=precision, preferred_element_type=jnp.float32
    )


def spread(value, row):
    return jnp.broadcast_to(value[row : row + 1, :], value.shape)


def lane_spread(value, lane):
    return jnp.broadcast_to(value[:, lane : lane + 1], value.shape)


def total(terms):
    while len(terms) > 1:
        terms = [a + b for a, b in zip(terms[::2], terms[1::2])] + terms[len(terms) // 2 * 2 :]
    return terms[0]


def factor_block(work):
    size = work.shape[0]
    lanes = lax.broadcasted_iota(jnp.int32, (8, size), 1)
    subs = lax.broadcasted_iota(jnp.int32, (8, size), 0)
    first = work[pl.ds(0, 8), :]
    cols = [lane_spread(first, j) for j in range(8)]
    for step in range(size // 8):
        base = 8 * step
        inside = (lanes >= base) & (lanes < base + 8)
        last = step + 1 == size // 8
        below = {
            other: work[pl.ds(8 * other, 8), :] for other in range(step + 1, size // 8)
        }
        beside = {
            other: [lane_spread(rows, base + j) for j in range(8)] for other, rows in below.items()
        }
        ratio, recip = {}, []
        for j in range(8):
            pivot = spread(cols[j], j)
            pivots = pivot if j == 0 else jnp.where(subs == j, pivot, pivots)
            recip.append(1.0 / pivot)
            for k in range(j + 1, 8):
                ratio[j, k] = spread(cols[j], k) * recip[j]
                cols[k] = cols[k] - cols[j] * ratio[j, k]
        if not last:
            near = list(beside[step + 1])
            for j in range(8):
                for k in range(j + 1, 8):
                    near[k] = near[k] - near[j] * ratio[j, k]
            own = [lane_spread(below[step + 1], base + 8 + i) for i in range(8)]
            shares = [near[j] * recip[j] for j in range(8)]
            own = [
                own[i] - total([near[j] * spread(shares[j], i) for j in range(8)]) for i in range(8)
            ]
        row = work[pl.ds(base, 8), :]
        row = jnp.where(inside, jnp.where(lanes - base == subs, 1.0, 0.0), row)
        solved = []
        for j in range(8):
            solved.append(spread(row, j) * recip[j])
            if j < 7:
                row = row - jnp.where(subs > j, cols[j], 0.0) * solved[j]
        work[pl.ds(base, 8), :] = row * lax.rsqrt(pivots)
        for j in reversed(range(7)):
            solved[j] = solved[j] - total([ratio[j, k] * solved[k] for k in range(j + 1, 8)])
        for other, rows in below.items():
            work[pl.ds(8 * other, 8), :] = jnp.where(inside, 0.0, rows) - total(
                [beside[other][j] * solved[j] for j in range(8)]
            )
        if not last:
            cols = own


def tril(value):
    rows = lax.broadcasted_iota(jnp.int32, value.shape, 0)
    return jnp.where(lax.broadcasted_iota(jnp.int32, value.shape, 1) <= rows, value, 0.0)


def factor_inverse(gram, work):
    size = gram.shape[0]
    count = size // BLOCK

    def step(index, carry):
        start = pl.multiple_of(index * BLOCK, BLOCK)
        here = pl.ds(start, BLOCK)
        work[...] = gram[here, here]
        factor_block(work)
        inverse = tril(work[...])
        gram[here, here] = jnp.eye(BLOCK, dtype=jnp.float32)
        for block in range(count):

            @pl.when(index == block)
            def _():
                low = BLOCK * block
                rest = size - low - BLOCK
                row = dot(inverse, gram[pl.ds(low, BLOCK), :])
                gram[pl.ds(low, BLOCK), :] = row
                if rest:
                    turned = row[:, low + BLOCK :].T
                    gram[pl.ds(low + BLOCK, rest), pl.ds(low, BLOCK)] = jnp.zeros(
                        (rest, BLOCK), jnp.float32
                    )
                    for other in range(0, rest, BLOCK):
                        rows = pl.ds(low + BLOCK + other, BLOCK)
                        gram[rows, :] = gram[rows, :] - dot(turned[other : other + BLOCK], row)

        return carry

    lax.fori_loop(0, count, step, 0)
    gram[...] = tril(gram[...])


def diagonal(value):
    rows = lax.broadcasted_iota(jnp.int32, value.shape, 0)
    cols = lax.broadcasted_iota(jnp.int32, value.shape, 1)
    return rows == cols


def half(value, offset=0):
    rows = lax.broadcasted_iota(jnp.int32, value.shape, 0) + offset
    cols = lax.broadcasted_iota(jnp.int32, value.shape, 1)
    return jnp.where(rows > cols, value, jnp.where(rows == cols, 0.5 * value, 0.0))


def split(value, parts):
    pieces = []
    for _ in range(parts):
        pieces.append(value.astype(jnp.bfloat16))
        value = value - pieces[-1].astype(jnp.float32)
    return pieces


def dot3(left, right, contract=((1,), (0,))):
    left_top, left_low = split(left, 2)
    right_top, right_low = split(right, 2)
    small = dot(left_low, right_top, contract, None) + dot(left_top, right_low, contract, None)
    return dot(left_top, right_top, contract, None) + small


def outer(left, right):
    a, b, c = split(left, 3)
    d, e, f = split(right, 3)
    left = jnp.concatenate([a, a, b, a, c, b], axis=0).astype(jnp.float32)
    right = jnp.concatenate([d, e, d, f, d, e], axis=0)
    return dot(left.T.astype(jnp.bfloat16), right, precision=None)


NT = ((1,), (1,))
STOP = 1e-5
NEAR = 0.2
BOUND = 1e30
SHIFT = 4e-6


def step_inverse(low, inverse):
    mid = low.shape[0] // 2
    inverse_top, inverse_low = inverse[:mid, :mid], inverse[...]
    inverse[:mid, :mid] = inverse_top - dot3(low[:mid, :mid], inverse_top)
    inverse[mid:, :] = inverse_low[mid:] - dot3(low[mid:], inverse_low)


def rotation(coeffs_ref, gram_ref, squares_ref, inverse, second, upper, work):
    coeffs = coeffs_ref[...]
    mid = coeffs.shape[1] // 2
    square = outer(coeffs, coeffs)
    upper[...] = square + jnp.where(diagonal(square), squares_ref[...], 0.0)

    def first_gram():
        extra = outer(coeffs, dot(gram_ref[...], coeffs))
        second[:mid, :] = dot(upper[:mid, :], upper[...]) + extra[:mid]
        second[mid:, mid:] = dot(upper[mid:, :], upper[:, mid:]) + extra[mid:, mid:]

    first_gram()

    def far(carry):
        return jnp.logical_not(carry[1] < NEAR) & (carry[0] < 8)

    def factor_pass(carry):
        count, _, fresh = carry
        factor_inverse(second, work)

        @pl.when(fresh == 1)
        def _():
            inverse[...] = second[...]

        @pl.when(fresh == 0)
        def _():
            inverse[...] = dot(second[...], inverse[...])

        second[:mid, :] = dot(inverse[:mid, :mid], upper[:mid, :])
        second[mid:, :] = dot(inverse[mid:, :], upper[...])
        part = dot3(inverse[...], coeffs, NT)
        side = dot3(part, gram_ref[...])
        stacked = second[...]
        gram_low = dot3(stacked[mid:], stacked, NT) + dot3(side[mid:], part, NT)
        gram_top = dot3(stacked[:mid], stacked[:mid], NT) + dot3(side[:mid], part[:mid], NT)
        second[:mid, :mid] = gram_top
        second[mid:, :] = gram_low
        second[:mid, mid:] = gram_low[:, :mid].T
        rest = second[...] - jnp.where(diagonal(square), 1.0, 0.0)
        size = jnp.sum(rest * rest)
        failed = jnp.logical_not(size < BOUND)

        @pl.when(failed)
        def _():
            first_gram()
            ends = jnp.where(diagonal(square), second[...], 0.0)
            second[...] = second[...] + jnp.where(diagonal(square), SHIFT * jnp.max(ends), 0.0)

        return count + 1, size, failed.astype(jnp.int32)

    _, size, _ = lax.while_loop(far, factor_pass, (jnp.int32(0), jnp.float32(BOUND), jnp.int32(1)))

    second[...] = second[...] - jnp.where(diagonal(square), 1.0, 0.0)

    def more(carry):
        return (carry[0] >= STOP) & (carry[1] < 16)

    def newton(carry):
        rest = second[...]
        low = half(rest)
        step_inverse(low, inverse)
        mixed = dot3(low, rest)
        rest = dot3(low + mixed, low, NT) - mixed - mixed.T
        second[...] = rest
        return jnp.sum(rest * rest), carry[1] + 1

    lax.while_loop(more, newton, (size, jnp.int32(0)))
    step_inverse(half(second[...]), inverse)


def update_kernel(
    coeffs_ref, gram_ref, squares_ref, snaps_ref, basis_hbm, out_hbm,
    inverse, second, upper, work, basis, out, loaded, stored,
):
    rows, modes = basis.shape
    snaps = coeffs_ref.shape[0]
    mid = modes // 2
    load = pltpu.make_async_copy(basis_hbm, basis, loaded)
    load.start()
    rotation(coeffs_ref, gram_ref, squares_ref, inverse, second, upper, work)
    final = inverse[...]
    turn_top, turn_low = split(final * squares_ref[...], 2)
    across_top, across_low = split(dot(final, coeffs_ref[...], NT).T, 2)
    across = jnp.concatenate([across_top, across_low, across_top], axis=0)
    chunk = chunk_of(rows)
    load.wait()
    copies = []
    for start in range(0, rows, chunk):
        here = pl.ds(start, chunk)
        snaps_top, snaps_low = split(snaps_ref[:, pl.ds(start, chunk)], 2)
        mixed = jnp.concatenate([snaps_top, snaps_top, snaps_low], axis=0).astype(jnp.float32)
        base = dot(mixed.T.astype(jnp.bfloat16), across, precision=None)
        top, low = split(basis[here, :], 2)
        for cols, depth in ((slice(0, mid), mid), (slice(mid, modes), modes)):
            value = base[:, cols]
            for a, b in ((low, turn_top), (top, turn_low), (top, turn_top)):
                value = value + dot(a[:, :depth], b[cols, :depth], NT, None)
            out[here, cols] = value.astype(out.dtype)
        copies.append(pltpu.make_async_copy(out.at[here, :], out_hbm.at[here, :], stored.at[start // chunk]))
        copies[-1].start()
    for copy in copies:
        copy.wait()


def chunk_of(rows):
    for chunk in (640, 512, 384, 256, 128):
        if rows % chunk == 0:
            return chunk
    return rows


def updated_basis(coeffs, gram_res, squares, snap_rows, old_basis):
    rows, modes = old_basis.shape
    whole = pltpu.VMEM((modes, modes), jnp.float32)
    spec = pl.BlockSpec(memory_space=pltpu.VMEM)
    far = pl.BlockSpec(memory_space=pl.ANY)
    return pl.pallas_call(
        update_kernel,
        out_shape=jax.ShapeDtypeStruct((rows, modes), jnp.bfloat16),
        in_specs=[spec] * 4 + [far],
        out_specs=far,
        scratch_shapes=[
            whole, whole, whole, pltpu.VMEM((BLOCK, BLOCK), jnp.float32),
            pltpu.VMEM((rows, modes), jnp.float32), pltpu.VMEM((rows, modes), jnp.bfloat16),
            pltpu.SemaphoreType.DMA, pltpu.SemaphoreType.DMA((rows // chunk_of(rows),)),
        ],
        compiler_params=pltpu.CompilerParams(vmem_limit_bytes=48 * 1024 * 1024),
    )(coeffs, gram_res, squares, snap_rows, old_basis)


HIGH = lax.Precision.HIGH


def mat(left, right, contract, precision=HIGH):
    return lax.dot_general(
        left, right, (contract, ((), ())), precision=precision, preferred_element_type=jnp.float32
    )


def pair_rounds():
    rounds = []
    for name in ("slab", "tile"):
        size = lax.axis_size(name)
        step = 1
        while step < size:
            rounds.append((name, [(i, i ^ step) for i in range(size)]))
            step *= 2
    return rounds


def sum_all(part):
    for name, pairs in pair_rounds():
        part = part + lax.ppermute(part, name, pairs)
    return part


def sum_all_halved(part):
    rounds = pair_rounds()
    half_rows = part.shape[0] // 2
    first = lax.axis_index(rounds[0][0]) % 2 == 0
    top, low = part[:half_rows], part[half_rows:]
    kept = jnp.where(first, top, low) + lax.ppermute(jnp.where(first, low, top), *rounds[0])
    for name, pairs in rounds[1:]:
        kept = kept + lax.ppermute(kept, name, pairs)
    other = lax.ppermute(kept, *rounds[0])
    return jnp.concatenate([jnp.where(first, kept, other), jnp.where(first, other, kept)], axis=0)


def local(snapshots, old_basis, sing_values):
    snap_rows = lax.all_to_all(snapshots, "tile", split_axis=1, concat_axis=0, tiled=True)
    cell_count = old_basis.shape[0] * lax.axis_size("tile") * lax.axis_size("slab")
    weight_cell = 1.0 / cell_count
    coeffs = sum_all_halved(mat(snap_rows, old_basis, ((1,), (0,))) * weight_cell)
    resid = snap_rows - mat(coeffs, old_basis, ((1,), (1,)))
    gram_res = sum_all(mat(resid, resid, ((1,), (1,))) * weight_cell)
    squares = (sing_values * sing_values)[None, :]
    return updated_basis(coeffs, gram_res, squares, snap_rows, old_basis)


def solution(mesh):
    placed = (P("tile", "slab"), P(("slab", "tile"), None), P())
    return jax.shard_map(
        local, mesh=mesh, in_specs=placed, out_specs=P(("slab", "tile"), None), check_vma=False
    )
```

```python
import functools

import jax
import jax.numpy as jnp
from jax import lax
from jax.experimental import pallas as pl
from jax.experimental.pallas import tpu as pltpu
from jax.sharding import PartitionSpec as P

HIGHEST = lax.Precision.HIGHEST
BLOCK = 128


def dot(left, right, contract=((1,), (0,)), precision=HIGHEST):
    return lax.dot_general(
        left, right, (contract, ((), ())), precision=precision, preferred_element_type=jnp.float32
    )


def spread(value, row):
    return jnp.broadcast_to(value[row : row + 1, :], value.shape)


def lane_spread(value, lane):
    return jnp.broadcast_to(value[:, lane : lane + 1], value.shape)


def total(terms):
    while len(terms) > 1:
        terms = [a + b for a, b in zip(terms[::2], terms[1::2])] + terms[len(terms) // 2 * 2 :]
    return terms[0]


def factor_block(work):
    size = work.shape[0]
    lanes = lax.broadcasted_iota(jnp.int32, (8, size), 1)
    subs = lax.broadcasted_iota(jnp.int32, (8, size), 0)
    first = work[pl.ds(0, 8), :]
    cols = [lane_spread(first, j) for j in range(8)]
    for step in range(size // 8):
        base = 8 * step
        inside = (lanes >= base) & (lanes < base + 8)
        last = step + 1 == size // 8
        below = {
            other: work[pl.ds(8 * other, 8), :] for other in range(step + 1, size // 8)
        }
        beside = {
            other: [lane_spread(rows, base + j) for j in range(8)] for other, rows in below.items()
        }
        ratio, recip = {}, []
        for j in range(8):
            pivot = spread(cols[j], j)
            pivots = pivot if j == 0 else jnp.where(subs == j, pivot, pivots)
            recip.append(1.0 / pivot)
            for k in range(j + 1, 8):
                ratio[j, k] = spread(cols[j], k) * recip[j]
                cols[k] = cols[k] - cols[j] * ratio[j, k]
        if not last:
            near = list(beside[step + 1])
            for j in range(8):
                for k in range(j + 1, 8):
                    near[k] = near[k] - near[j] * ratio[j, k]
            own = [lane_spread(below[step + 1], base + 8 + i) for i in range(8)]
            shares = [near[j] * recip[j] for j in range(8)]
            own = [
                own[i] - total([near[j] * spread(shares[j], i) for j in range(8)]) for i in range(8)
            ]
        row = work[pl.ds(base, 8), :]
        row = jnp.where(inside, jnp.where(lanes - base == subs, 1.0, 0.0), row)
        solved = []
        for j in range(8):
            solved.append(spread(row, j) * recip[j])
            if j < 7:
                row = row - jnp.where(subs > j, cols[j], 0.0) * solved[j]
        work[pl.ds(base, 8), :] = row * lax.rsqrt(pivots)
        for j in reversed(range(7)):
            solved[j] = solved[j] - total([ratio[j, k] * solved[k] for k in range(j + 1, 8)])
        for other, rows in below.items():
            work[pl.ds(8 * other, 8), :] = jnp.where(inside, 0.0, rows) - total(
                [beside[other][j] * solved[j] for j in range(8)]
            )
        if not last:
            cols = own


def tril(value):
    rows = lax.broadcasted_iota(jnp.int32, value.shape, 0)
    return jnp.where(lax.broadcasted_iota(jnp.int32, value.shape, 1) <= rows, value, 0.0)


def split(value, parts):
    pieces = []
    for _ in range(parts):
        pieces.append(value.astype(jnp.bfloat16))
        value = value - pieces[-1].astype(jnp.float32)
    return pieces


def block_dot(left, right):
    a, b, c = split(left, 3)
    d, e, f = split(right, 3)
    both = jnp.concatenate([d, e], axis=0)
    value = dot(jnp.concatenate([a, c], axis=1), jnp.concatenate([f, d], axis=0), precision=None)
    value = value + dot(jnp.concatenate([b, b], axis=1), both, precision=None)
    return value + dot(jnp.concatenate([a, a], axis=1), both, precision=None)


def factor_inverse(gram, work):
    size = gram.shape[0]
    count = size // BLOCK

    def step(index, carry):
        start = pl.multiple_of(index * BLOCK, BLOCK)
        here = pl.ds(start, BLOCK)
        work[...] = gram[here, here]
        factor_block(work)
        inverse = tril(work[...])
        gram[here, here] = jnp.eye(BLOCK, dtype=jnp.float32)
        for block in range(count):

            @pl.when(index == block)
            def _():
                low = BLOCK * block
                high = low + BLOCK
                row = block_dot(inverse, gram[low:high, :])
                gram[low:high, :] = row
                if high < size:
                    gram[high:, low:high] = jnp.zeros((size - high, BLOCK), jnp.float32)
                    gram[high:, :] = gram[high:, :] - block_dot(row[:, high:].T, row)

        return carry

    lax.fori_loop(0, count, step, 0)
    gram[...] = tril(gram[...])


def diagonal(value):
    rows = lax.broadcasted_iota(jnp.int32, value.shape, 0)
    cols = lax.broadcasted_iota(jnp.int32, value.shape, 1)
    return rows == cols


def half(value, offset=0):
    rows = lax.broadcasted_iota(jnp.int32, value.shape, 0) + offset
    cols = lax.broadcasted_iota(jnp.int32, value.shape, 1)
    return jnp.where(rows > cols, value, jnp.where(rows == cols, 0.5 * value, 0.0))


def dot3(left, right, contract=((1,), (0,))):
    left_top, left_low = split(left, 2)
    right_top, right_low = split(right, 2)
    small = dot(left_low, right_top, contract, None) + dot(left_top, right_low, contract, None)
    return dot(left_top, right_top, contract, None) + small


def outer(left, right):
    a, b, c = split(left, 3)
    d, e, f = split(right, 3)
    left = jnp.concatenate([a, a, b, a, c, b], axis=0).astype(jnp.float32)
    right = jnp.concatenate([d, e, d, f, d, e], axis=0)
    return dot(left.T.astype(jnp.bfloat16), right, precision=None)


NT = ((1,), (1,))
STOP = 1e-5
NEAR = 0.2
BOUND = 1e30
SHIFT = 4e-6


def step_inverse(low, inverse):
    mid = low.shape[0] // 2
    inverse_top, inverse_low = inverse[:mid, :mid], inverse[...]
    inverse[:mid, :mid] = inverse_top - dot3(low[:mid, :mid], inverse_top)
    inverse[mid:, :] = inverse_low[mid:] - dot3(low[mid:], inverse_low)


def opening_kernel(coeffs_ref, squares_ref, upper, square):
    coeffs = coeffs_ref[...]
    mid = coeffs.shape[1] // 2
    value = outer(coeffs, coeffs)
    upper[...] = value + jnp.where(diagonal(value), squares_ref[...], 0.0)
    square[:mid, :] = dot(upper[:mid, :], upper[...])
    square[mid:, :mid] = jnp.zeros((mid, mid), jnp.float32)
    square[mid:, mid:] = dot(upper[mid:, :], upper[:, mid:])


def opening(coeffs, squares):
    modes = coeffs.shape[1]
    spec = pl.BlockSpec(memory_space=pltpu.VMEM)
    shape = jax.ShapeDtypeStruct((modes, modes), jnp.float32)
    return pl.pallas_call(
        opening_kernel, out_shape=(shape, shape), in_specs=[spec] * 2, out_specs=(spec, spec),
        cost_estimate=pl.CostEstimate(
            flops=12 * modes**3, bytes_accessed=8 * modes**2, transcendentals=0
        ),
    )(coeffs, squares)


def coeffs_kernel(weight, snaps_ref, basis_ref, out_ref):
    rows = basis_ref.shape[0]
    chunk = chunk_of(rows)
    total_value = None
    for start in range(0, rows, chunk):
        here = pl.ds(start, chunk)
        term = dot3(snaps_ref[:, here], basis_ref[here, :])
        total_value = term if total_value is None else total_value + term
    out_ref[...] = total_value * weight


def local_coeffs(snap_rows, old_basis, weight):
    spec = pl.BlockSpec(memory_space=pltpu.VMEM)
    return pl.pallas_call(
        functools.partial(coeffs_kernel, weight),
        out_shape=jax.ShapeDtypeStruct((snap_rows.shape[0], old_basis.shape[1]), jnp.float32),
        in_specs=[spec] * 2, out_specs=spec,
    )(snap_rows, old_basis)


def rotation(coeffs_ref, gram_ref, upper, square_ref, inverse, second, work):
    coeffs = coeffs_ref[...]
    mid = coeffs.shape[1] // 2
    square = square_ref

    def first_gram():
        second[...] = square_ref[...] + outer(coeffs, dot(gram_ref[...], coeffs))

    first_gram()

    def far(carry):
        return jnp.logical_not(carry[1] < NEAR) & (carry[0] < 8)

    def factor_pass(carry):
        count, _, fresh = carry
        factor_inverse(second, work)

        @pl.when(fresh == 1)
        def _():
            inverse[...] = second[...]

        @pl.when(fresh == 0)
        def _():
            inverse[...] = dot(second[...], inverse[...])

        second[:mid, :] = dot(inverse[:mid, :mid], upper[:mid, :])
        second[mid:, :] = dot(inverse[mid:, :], upper[...])
        part = dot3(inverse[...], coeffs, NT)
        side = dot3(part, gram_ref[...])
        stacked = second[...]
        gram_low = dot3(stacked[mid:], stacked, NT) + dot3(side[mid:], part, NT)
        gram_top = dot3(stacked[:mid], stacked[:mid], NT) + dot3(side[:mid], part[:mid], NT)
        second[:mid, :mid] = gram_top
        second[mid:, :] = gram_low
        second[:mid, mid:] = gram_low[:, :mid].T
        rest = second[...] - jnp.where(diagonal(square), 1.0, 0.0)
        size = jnp.sum(rest * rest)
        failed = jnp.logical_not(size < BOUND)

        @pl.when(failed)
        def _():
            first_gram()
            ends = jnp.where(diagonal(square), second[...], 0.0)
            second[...] = second[...] + jnp.where(diagonal(square), SHIFT * jnp.max(ends), 0.0)

        return count + 1, size, failed.astype(jnp.int32)

    _, size, _ = lax.while_loop(far, factor_pass, (jnp.int32(0), jnp.float32(BOUND), jnp.int32(1)))

    second[...] = second[...] - jnp.where(diagonal(square), 1.0, 0.0)

    def more(carry):
        return (carry[0] >= STOP) & (carry[1] < 16)

    def newton(carry):
        rest = second[...]
        low = half(rest)
        step_inverse(low, inverse)
        mixed = dot3(low, rest)
        rest = dot3(low + mixed, low, NT) - mixed - mixed.T
        second[...] = rest
        return jnp.sum(rest * rest), carry[1] + 1

    lax.while_loop(more, newton, (size, jnp.int32(0)))
    step_inverse(half(second[...]), inverse)


def update_kernel(
    coeffs_ref, gram_ref, squares_ref, upper, square_ref, snaps_ref, basis_hbm, out_hbm,
    inverse, second, work, basis, out, loaded, stored,
):
    rows, modes = basis.shape
    snaps = coeffs_ref.shape[0]
    mid = modes // 2
    load = pltpu.make_async_copy(basis_hbm, basis, loaded)
    load.start()
    rotation(coeffs_ref, gram_ref, upper, square_ref, inverse, second, work)
    final = inverse[...]
    turn_top, turn_low = split(final * squares_ref[...], 2)
    across_top, across_low = split(dot(final, coeffs_ref[...], NT).T, 2)
    across = jnp.concatenate([across_top, across_low, across_top], axis=0)
    chunk = chunk_of(rows)
    load.wait()
    copies = []
    for start in range(0, rows, chunk):
        here = pl.ds(start, chunk)
        snaps_top, snaps_low = split(snaps_ref[:, pl.ds(start, chunk)], 2)
        mixed = jnp.concatenate([snaps_top, snaps_top, snaps_low], axis=0).astype(jnp.float32)
        base = dot(mixed.T.astype(jnp.bfloat16), across, precision=None)
        top, low = split(basis[here, :], 2)
        for cols, depth in ((slice(0, mid), mid), (slice(mid, modes), modes)):
            value = base[:, cols]
            for a, b in ((low, turn_top), (top, turn_low), (top, turn_top)):
                value = value + dot(a[:, :depth], b[cols, :depth], NT, None)
            out[here, cols] = value.astype(out.dtype)
        copies.append(pltpu.make_async_copy(out.at[here, :], out_hbm.at[here, :], stored.at[start // chunk]))
        copies[-1].start()
    for copy in copies:
        copy.wait()


def chunk_of(rows):
    for chunk in (640, 512, 384, 256, 128):
        if rows % chunk == 0:
            return chunk
    return rows


def updated_basis(coeffs, gram_res, squares, upper, square, snap_rows, old_basis):
    rows, modes = old_basis.shape
    whole = pltpu.VMEM((modes, modes), jnp.float32)
    spec = pl.BlockSpec(memory_space=pltpu.VMEM)
    far = pl.BlockSpec(memory_space=pl.ANY)
    return pl.pallas_call(
        update_kernel,
        out_shape=jax.ShapeDtypeStruct((rows, modes), jnp.bfloat16),
        in_specs=[spec] * 6 + [far],
        out_specs=far,
        scratch_shapes=[
            whole, whole, pltpu.VMEM((BLOCK, BLOCK), jnp.float32),
            pltpu.VMEM((rows, modes), jnp.float32), pltpu.VMEM((rows, modes), jnp.bfloat16),
            pltpu.SemaphoreType.DMA, pltpu.SemaphoreType.DMA((rows // chunk_of(rows),)),
        ],
        compiler_params=pltpu.CompilerParams(vmem_limit_bytes=48 * 1024 * 1024),
    )(coeffs, gram_res, squares, upper, square, snap_rows, old_basis)


HIGH = lax.Precision.HIGH


def mat(left, right, contract, precision=HIGH):
    return lax.dot_general(
        left, right, (contract, ((), ())), precision=precision, preferred_element_type=jnp.float32
    )


AXES = ("tile", "slab")


def exchange(part, mask):
    count = lax.axis_size(AXES[0]) * lax.axis_size(AXES[1])
    return lax.ppermute(part, AXES, [(i, i ^ mask) for i in range(count)])


def sum_rounds():
    count = lax.axis_size(AXES[0]) * lax.axis_size(AXES[1])
    rounds, bit = [], 2
    while bit < count:
        rounds.append([bit, 2 * bit, 3 * bit] if 2 * bit < count else [bit])
        bit *= 4
    return rounds


def sum_round(part, masks):
    others = [exchange(part, mask) for mask in masks]
    if len(others) == 1:
        return part + others[0]
    return (part + others[0]) + (others[1] + others[2])


def sum_all(part):
    part = part + exchange(part, 1)
    for masks in sum_rounds():
        part = sum_round(part, masks)
    return part


def sum_all_halved(part):
    half_rows = part.shape[0] // 2
    first = lax.axis_index(AXES[1]) % 2 == 0
    top, low = part[:half_rows], part[half_rows:]
    kept = jnp.where(first, top, low) + exchange(jnp.where(first, low, top), 1)
    for masks in sum_rounds():
        kept = sum_round(kept, masks)
    other = exchange(kept, 1)
    return jnp.concatenate([jnp.where(first, kept, other), jnp.where(first, other, kept)], axis=0)


def local(snapshots, old_basis, sing_values):
    snap_rows = lax.all_to_all(snapshots, "tile", split_axis=1, concat_axis=0, tiled=True)
    cell_count = old_basis.shape[0] * lax.axis_size("tile") * lax.axis_size("slab")
    weight_cell = 1.0 / cell_count
    coeffs = sum_all_halved(local_coeffs(snap_rows, old_basis, weight_cell))
    resid = snap_rows - mat(coeffs, old_basis, ((1,), (1,)))
    gram_part = mat(resid, resid, ((1,), (1,))) * weight_cell
    squares = (sing_values * sing_values)[None, :]
    gram_res = sum_all(gram_part)
    upper, square = opening(lax.optimization_barrier((coeffs, gram_part))[0], squares)
    return updated_basis(coeffs, gram_res, squares, upper, square, snap_rows, old_basis)


def solution(mesh):
    placed = (P("tile", "slab"), P(("slab", "tile"), None), P())
    return jax.shard_map(
        local, mesh=mesh, in_specs=placed, out_specs=P(("slab", "tile"), None), check_vma=False
    )
```

```python
import functools

import jax
import jax.numpy as jnp
from jax import lax
from jax.experimental import pallas as pl
from jax.experimental.pallas import tpu as pltpu
from jax.sharding import PartitionSpec as P

HIGHEST = lax.Precision.HIGHEST
BLOCK = 128
VMEM = 28 * 1024 * 1024


def dot(left, right, contract=((1,), (0,)), precision=HIGHEST):
    return lax.dot_general(
        left, right, (contract, ((), ())), precision=precision, preferred_element_type=jnp.float32
    )


def spread(value, row):
    return jnp.broadcast_to(value[row : row + 1, :], value.shape)


def lane_spread(value, lane):
    return jnp.broadcast_to(value[:, lane : lane + 1], value.shape)


def total(terms):
    while len(terms) > 1:
        terms = [a + b for a, b in zip(terms[::2], terms[1::2])] + terms[len(terms) // 2 * 2 :]
    return terms[0]


def factor_block(work):
    size = work.shape[0]
    lanes = lax.broadcasted_iota(jnp.int32, (8, size), 1)
    subs = lax.broadcasted_iota(jnp.int32, (8, size), 0)
    first = work[pl.ds(0, 8), :]
    cols = [lane_spread(first, j) for j in range(8)]
    for step in range(size // 8):
        base = 8 * step
        inside = (lanes >= base) & (lanes < base + 8)
        last = step + 1 == size // 8
        below = {
            other: work[pl.ds(8 * other, 8), :] for other in range(step + 1, size // 8)
        }
        beside = {
            other: [lane_spread(rows, base + j) for j in range(8)] for other, rows in below.items()
        }
        ratio, recip = {}, []
        for j in range(8):
            pivot = spread(cols[j], j)
            pivots = pivot if j == 0 else jnp.where(subs == j, pivot, pivots)
            recip.append(1.0 / pivot)
            for k in range(j + 1, 8):
                ratio[j, k] = spread(cols[j], k) * recip[j]
                cols[k] = cols[k] - cols[j] * ratio[j, k]
        if not last:
            near = list(beside[step + 1])
            for j in range(8):
                for k in range(j + 1, 8):
                    near[k] = near[k] - near[j] * ratio[j, k]
            own = [lane_spread(below[step + 1], base + 8 + i) for i in range(8)]
            shares = [near[j] * recip[j] for j in range(8)]
            own = [
                own[i] - total([near[j] * spread(shares[j], i) for j in range(8)]) for i in range(8)
            ]
        row = work[pl.ds(base, 8), :]
        row = jnp.where(inside, jnp.where(lanes - base == subs, 1.0, 0.0), row)
        solved = []
        for j in range(8):
            solved.append(spread(row, j) * recip[j])
            if j < 7:
                row = row - jnp.where(subs > j, cols[j], 0.0) * solved[j]
        work[pl.ds(base, 8), :] = row * lax.rsqrt(pivots)
        for j in reversed(range(7)):
            solved[j] = solved[j] - total([ratio[j, k] * solved[k] for k in range(j + 1, 8)])
        for other, rows in below.items():
            work[pl.ds(8 * other, 8), :] = jnp.where(inside, 0.0, rows) - total(
                [beside[other][j] * solved[j] for j in range(8)]
            )
        if not last:
            cols = own


def tril(value):
    rows = lax.broadcasted_iota(jnp.int32, value.shape, 0)
    return jnp.where(lax.broadcasted_iota(jnp.int32, value.shape, 1) <= rows, value, 0.0)


def split(value, parts):
    pieces = []
    for _ in range(parts):
        pieces.append(value.astype(jnp.bfloat16))
        value = value - pieces[-1].astype(jnp.float32)
    return pieces


def block_dot(left, right):
    a, b, c = split(left, 3)
    d, e, f = split(right, 3)
    both = jnp.concatenate([d, e], axis=0)
    value = dot(jnp.concatenate([a, c], axis=1), jnp.concatenate([f, d], axis=0), precision=None)
    value = value + dot(jnp.concatenate([b, b], axis=1), both, precision=None)
    return value + dot(jnp.concatenate([a, a], axis=1), both, precision=None)


def factor_inverse(gram, work):
    size = gram.shape[0]
    count = size // BLOCK

    def step(index, carry):
        start = pl.multiple_of(index * BLOCK, BLOCK)
        here = pl.ds(start, BLOCK)
        work[...] = gram[here, here]
        factor_block(work)
        inverse = tril(work[...])
        gram[here, here] = jnp.eye(BLOCK, dtype=jnp.float32)
        for block in range(count):

            @pl.when(index == block)
            def _():
                low = BLOCK * block
                high = low + BLOCK
                row = block_dot(inverse, gram[low:high, :])
                gram[low:high, :] = row
                if high < size:
                    gram[high:, low:high] = jnp.zeros((size - high, BLOCK), jnp.float32)
                    gram[high:, :] = gram[high:, :] - block_dot(row[:, high:].T, row)

        return carry

    lax.fori_loop(0, count, step, 0)
    gram[...] = tril(gram[...])


def diagonal(value):
    rows = lax.broadcasted_iota(jnp.int32, value.shape, 0)
    cols = lax.broadcasted_iota(jnp.int32, value.shape, 1)
    return rows == cols


def half(value, offset=0):
    rows = lax.broadcasted_iota(jnp.int32, value.shape, 0) + offset
    cols = lax.broadcasted_iota(jnp.int32, value.shape, 1)
    return jnp.where(rows > cols, value, jnp.where(rows == cols, 0.5 * value, 0.0))


def dot3(left, right, contract=((1,), (0,))):
    left_top, left_low = split(left, 2)
    right_top, right_low = split(right, 2)
    small = dot(left_low, right_top, contract, None) + dot(left_top, right_low, contract, None)
    return dot(left_top, right_top, contract, None) + small


def outer(left, right):
    a, b, c = split(left, 3)
    d, e, f = split(right, 3)
    left = jnp.concatenate([a, a, b, a, c, b], axis=0).astype(jnp.float32)
    right = jnp.concatenate([d, e, d, f, d, e], axis=0)
    return dot(left.T.astype(jnp.bfloat16), right, precision=None)


NT = ((1,), (1,))
STOP = 1e-5
NEAR = 0.2
BOUND = 1e30
SHIFT = 4e-6


def step_inverse(low, inverse):
    mid = low.shape[0] // 2
    inverse_top, inverse_low = inverse[:mid, :mid], inverse[...]
    inverse[:mid, :mid] = inverse_top - dot3(low[:mid, :mid], inverse_top)
    inverse[mid:, :] = inverse_low[mid:] - dot3(low[mid:], inverse_low)


def opening_kernel(coeffs_ref, squares_ref, upper, square):
    coeffs = coeffs_ref[...]
    mid = coeffs.shape[1] // 2
    value = outer(coeffs, coeffs)
    upper[...] = value + jnp.where(diagonal(value), squares_ref[...], 0.0)
    square[:mid, :] = dot(upper[:mid, :], upper[...])
    square[mid:, :mid] = jnp.zeros((mid, mid), jnp.float32)
    square[mid:, mid:] = dot(upper[mid:, :], upper[:, mid:])


def opening(coeffs, squares):
    modes = coeffs.shape[1]
    spec = pl.BlockSpec(memory_space=pltpu.VMEM)
    shape = jax.ShapeDtypeStruct((modes, modes), jnp.float32)
    return pl.pallas_call(
        opening_kernel, out_shape=(shape, shape), in_specs=[spec] * 2, out_specs=(spec, spec),
        compiler_params=pltpu.CompilerParams(vmem_limit_bytes=VMEM),
        cost_estimate=pl.CostEstimate(
            flops=12 * modes**3, bytes_accessed=8 * modes**2, transcendentals=0
        ),
    )(coeffs, squares)


def rotation(coeffs_ref, gram_ref, upper, square_ref, inverse, second, work):
    coeffs = coeffs_ref[...]
    mid = coeffs.shape[1] // 2
    square = square_ref

    def first_gram():
        second[...] = square_ref[...] + outer(coeffs, dot(gram_ref[...], coeffs))

    first_gram()

    def far(carry):
        return jnp.logical_not(carry[1] < NEAR) & (carry[0] < 8)

    def factor_pass(carry):
        count, _, fresh = carry
        factor_inverse(second, work)

        @pl.when(fresh == 1)
        def _():
            inverse[...] = second[...]

        @pl.when(fresh == 0)
        def _():
            inverse[...] = dot(second[...], inverse[...])

        second[:mid, :] = dot(inverse[:mid, :mid], upper[:mid, :])
        second[mid:, :] = dot(inverse[mid:, :], upper[...])
        part = dot3(inverse[...], coeffs, NT)
        side = dot3(part, gram_ref[...])
        stacked = second[...]
        gram_low = dot3(stacked[mid:], stacked, NT) + dot3(side[mid:], part, NT)
        gram_top = dot3(stacked[:mid], stacked[:mid], NT) + dot3(side[:mid], part[:mid], NT)
        second[:mid, :mid] = gram_top
        second[mid:, :] = gram_low
        second[:mid, mid:] = gram_low[:, :mid].T
        rest = second[...] - jnp.where(diagonal(square), 1.0, 0.0)
        size = jnp.sum(rest * rest)
        failed = jnp.logical_not(size < BOUND)

        @pl.when(failed)
        def _():
            first_gram()
            ends = jnp.where(diagonal(square), second[...], 0.0)
            second[...] = second[...] + jnp.where(diagonal(square), SHIFT * jnp.max(ends), 0.0)

        return count + 1, size, failed.astype(jnp.int32)

    _, size, _ = lax.while_loop(far, factor_pass, (jnp.int32(0), jnp.float32(BOUND), jnp.int32(1)))

    second[...] = second[...] - jnp.where(diagonal(square), 1.0, 0.0)

    def more(carry):
        return (carry[0] >= STOP) & (carry[1] < 16)

    def newton(carry):
        rest = second[...]
        low = half(rest)
        step_inverse(low, inverse)
        mixed = dot3(low, rest)
        rest = dot3(low + mixed, low, NT) - mixed - mixed.T
        second[...] = rest
        return jnp.sum(rest * rest), carry[1] + 1

    lax.while_loop(more, newton, (size, jnp.int32(0)))
    step_inverse(half(second[...]), inverse)


def update_kernel(
    coeffs_ref, gram_ref, squares_ref, upper, square_ref, snaps_ref, basis_hbm, out_hbm,
    inverse, second, work, basis, out, loaded, stored,
):
    rows, modes = basis.shape
    snaps = coeffs_ref.shape[0]
    mid = modes // 2
    load = pltpu.make_async_copy(basis_hbm, basis, loaded)
    load.start()
    rotation(coeffs_ref, gram_ref, upper, square_ref, inverse, second, work)
    final = inverse[...]
    turn_top, turn_low = split(final * squares_ref[...], 2)
    across_top, across_low = split(dot(final, coeffs_ref[...], NT).T, 2)
    across = jnp.concatenate([across_top, across_low, across_top], axis=0)
    chunk = chunk_of(rows)
    load.wait()
    copies = []
    for start in range(0, rows, chunk):
        here = pl.ds(start, chunk)
        snaps_top, snaps_low = split(snaps_ref[:, pl.ds(start, chunk)], 2)
        mixed = jnp.concatenate([snaps_top, snaps_top, snaps_low], axis=0).astype(jnp.float32)
        base = dot(mixed.T.astype(jnp.bfloat16), across, precision=None)
        top, low = split(basis[here, :], 2)
        for cols, depth in ((slice(0, mid), mid), (slice(mid, modes), modes)):
            value = base[:, cols]
            for a, b in ((low, turn_top), (top, turn_low), (top, turn_top)):
                value = value + dot(a[:, :depth], b[cols, :depth], NT, None)
            out[here, cols] = value.astype(out.dtype)
        copies.append(pltpu.make_async_copy(out.at[here, :], out_hbm.at[here, :], stored.at[start // chunk]))
        copies[-1].start()
    for copy in copies:
        copy.wait()


def chunk_of(rows):
    for chunk in (640, 512, 384, 256, 128):
        if rows % chunk == 0:
            return chunk
    return rows


def updated_basis(coeffs, gram_res, squares, upper, square, snap_rows, old_basis):
    rows, modes = old_basis.shape
    whole = pltpu.VMEM((modes, modes), jnp.float32)
    spec = pl.BlockSpec(memory_space=pltpu.VMEM)
    far = pl.BlockSpec(memory_space=pl.ANY)
    return pl.pallas_call(
        update_kernel,
        out_shape=jax.ShapeDtypeStruct((rows, modes), jnp.bfloat16),
        in_specs=[spec] * 6 + [far],
        out_specs=far,
        scratch_shapes=[
            whole, whole, pltpu.VMEM((BLOCK, BLOCK), jnp.float32),
            pltpu.VMEM((rows, modes), jnp.float32), pltpu.VMEM((rows, modes), jnp.bfloat16),
            pltpu.SemaphoreType.DMA, pltpu.SemaphoreType.DMA((rows // chunk_of(rows),)),
        ],
        compiler_params=pltpu.CompilerParams(vmem_limit_bytes=VMEM),
    )(coeffs, gram_res, squares, upper, square, snap_rows, old_basis)


HIGH = lax.Precision.HIGH


def mat(left, right, contract, precision=HIGH):
    return lax.dot_general(
        left, right, (contract, ((), ())), precision=precision, preferred_element_type=jnp.float32
    )


AXES = ("tile", "slab")


def exchange(part, mask):
    count = lax.axis_size(AXES[0]) * lax.axis_size(AXES[1])
    return lax.ppermute(part, AXES, [(i, i ^ mask) for i in range(count)])


def sum_rounds():
    count = lax.axis_size(AXES[0]) * lax.axis_size(AXES[1])
    rounds, bit = [], 2
    while bit < count:
        rounds.append([bit, 2 * bit, 3 * bit] if 2 * bit < count else [bit])
        bit *= 4
    return rounds


def sum_round(part, masks):
    others = [exchange(part, mask) for mask in masks]
    if len(others) == 1:
        return part + others[0]
    return (part + others[0]) + (others[1] + others[2])


def sum_all(part):
    part = part + exchange(part, 1)
    for masks in sum_rounds():
        part = sum_round(part, masks)
    return part


def sum_all_halved(part):
    half_rows = part.shape[0] // 2
    first = lax.axis_index(AXES[1]) % 2 == 0
    top, low = part[:half_rows], part[half_rows:]
    kept = jnp.where(first, top, low) + exchange(jnp.where(first, low, top), 1)
    for masks in sum_rounds():
        kept = sum_round(kept, masks)
    other = exchange(kept, 1)
    return jnp.concatenate([jnp.where(first, kept, other), jnp.where(first, other, kept)], axis=0)


def local(snapshots, old_basis, sing_values):
    snap_rows = lax.all_to_all(snapshots, "tile", split_axis=1, concat_axis=0, tiled=True)
    cell_count = old_basis.shape[0] * lax.axis_size("tile") * lax.axis_size("slab")
    weight_cell = 1.0 / cell_count
    coeffs = sum_all_halved(mat(snap_rows, old_basis, ((1,), (0,))) * weight_cell)
    resid = snap_rows - mat(coeffs, old_basis, ((1,), (1,)))
    gram_part = mat(resid, resid, ((1,), (1,))) * weight_cell
    squares = (sing_values * sing_values)[None, :]
    gram_res = sum_all(gram_part)
    upper, square = opening(lax.optimization_barrier((coeffs, gram_part))[0], squares)
    return updated_basis(coeffs, gram_res, squares, upper, square, snap_rows, old_basis)


def solution(mesh):
    placed = (P("tile", "slab"), P(("slab", "tile"), None), P())
    return jax.shard_map(
        local, mesh=mesh, in_specs=placed, out_specs=P(("slab", "tile"), None), check_vma=False
    )
```

```python
import functools

import jax
import jax.numpy as jnp
from jax import lax
from jax.experimental import pallas as pl
from jax.experimental.pallas import tpu as pltpu
from jax.sharding import PartitionSpec as P

HIGHEST = lax.Precision.HIGHEST
BLOCK = 128
LANES = 128
VMEM = 28 * 1024 * 1024


def dot(left, right, contract=((1,), (0,)), precision=HIGHEST):
    return lax.dot_general(
        left, right, (contract, ((), ())), precision=precision, preferred_element_type=jnp.float32
    )


def spread(value, row):
    return jnp.broadcast_to(value[row : row + 1, :], value.shape)


def lane_spread(value, lane):
    return jnp.broadcast_to(value[:, lane : lane + 1], value.shape)


def total(terms):
    while len(terms) > 1:
        terms = [a + b for a, b in zip(terms[::2], terms[1::2])] + terms[len(terms) // 2 * 2 :]
    return terms[0]


def factor_block(work):
    size = work.shape[0]
    lanes = lax.broadcasted_iota(jnp.int32, (8, size), 1)
    subs = lax.broadcasted_iota(jnp.int32, (8, size), 0)
    first = work[pl.ds(0, 8), :]
    cols = [lane_spread(first, j) for j in range(8)]
    for step in range(size // 8):
        base = 8 * step
        inside = (lanes >= base) & (lanes < base + 8)
        last = step + 1 == size // 8
        below = {
            other: work[pl.ds(8 * other, 8), :] for other in range(step + 1, size // 8)
        }
        beside = {
            other: [lane_spread(rows, base + j) for j in range(8)] for other, rows in below.items()
        }
        ratio, recip = {}, []
        for j in range(8):
            pivot = spread(cols[j], j)
            pivots = pivot if j == 0 else jnp.where(subs == j, pivot, pivots)
            recip.append(1.0 / pivot)
            for k in range(j + 1, 8):
                ratio[j, k] = spread(cols[j], k) * recip[j]
                cols[k] = cols[k] - cols[j] * ratio[j, k]
        if not last:
            near = list(beside[step + 1])
            for j in range(8):
                for k in range(j + 1, 8):
                    near[k] = near[k] - near[j] * ratio[j, k]
            own = [lane_spread(below[step + 1], base + 8 + i) for i in range(8)]
            shares = [near[j] * recip[j] for j in range(8)]
            own = [
                own[i] - total([near[j] * spread(shares[j], i) for j in range(8)]) for i in range(8)
            ]
        row = work[pl.ds(base, 8), :]
        row = jnp.where(inside, jnp.where(lanes - base == subs, 1.0, 0.0), row)
        solved = []
        for j in range(8):
            solved.append(spread(row, j) * recip[j])
            if j < 7:
                row = row - jnp.where(subs > j, cols[j], 0.0) * solved[j]
        work[pl.ds(base, 8), :] = row * lax.rsqrt(pivots)
        for j in reversed(range(7)):
            solved[j] = solved[j] - total([ratio[j, k] * solved[k] for k in range(j + 1, 8)])
        for other, rows in below.items():
            work[pl.ds(8 * other, 8), :] = jnp.where(inside, 0.0, rows) - total(
                [beside[other][j] * solved[j] for j in range(8)]
            )
        if not last:
            cols = own


def tril(value):
    rows = lax.broadcasted_iota(jnp.int32, value.shape, 0)
    return jnp.where(lax.broadcasted_iota(jnp.int32, value.shape, 1) <= rows, value, 0.0)


def split(value, parts):
    pieces = []
    for _ in range(parts):
        pieces.append(value.astype(jnp.bfloat16))
        value = value - pieces[-1].astype(jnp.float32)
    return pieces


def block_dot(left, right):
    a, b, c = split(left, 3)
    d, e, f = split(right, 3)
    both = jnp.concatenate([d, e], axis=0)
    value = dot(jnp.concatenate([a, c], axis=1), jnp.concatenate([f, d], axis=0), precision=None)
    value = value + dot(jnp.concatenate([b, b], axis=1), both, precision=None)
    return value + dot(jnp.concatenate([a, a], axis=1), both, precision=None)


def factor_inverse(gram, work):
    size = gram.shape[0]
    count = size // BLOCK

    def step(index, carry):
        start = pl.multiple_of(index * BLOCK, BLOCK)
        here = pl.ds(start, BLOCK)
        work[...] = gram[here, here]
        factor_block(work)
        inverse = tril(work[...])
        gram[here, here] = jnp.eye(BLOCK, dtype=jnp.float32)
        for block in range(count):

            @pl.when(index == block)
            def _():
                low = BLOCK * block
                high = low + BLOCK
                row = block_dot(inverse, gram[low:high, :])
                gram[low:high, :] = row
                if high < size:
                    gram[high:, low:high] = jnp.zeros((size - high, BLOCK), jnp.float32)
                    gram[high:, :] = gram[high:, :] - block_dot(row[:, high:].T, row)

        return carry

    lax.fori_loop(0, count, step, 0)
    gram[...] = tril(gram[...])


def diagonal(value):
    rows = lax.broadcasted_iota(jnp.int32, value.shape, 0)
    cols = lax.broadcasted_iota(jnp.int32, value.shape, 1)
    return rows == cols


def half(value, offset=0):
    rows = lax.broadcasted_iota(jnp.int32, value.shape, 0) + offset
    cols = lax.broadcasted_iota(jnp.int32, value.shape, 1)
    return jnp.where(rows > cols, value, jnp.where(rows == cols, 0.5 * value, 0.0))


def dot3(left, right, contract=((1,), (0,))):
    left_top, left_low = split(left, 2)
    right_top, right_low = split(right, 2)
    small = dot(left_low, right_top, contract, None) + dot(left_top, right_low, contract, None)
    return dot(left_top, right_top, contract, None) + small


def outer(left, right):
    a, b, c = split(left, 3)
    d, e, f = split(right, 3)
    left = jnp.concatenate([a, a, b, a, c, b], axis=0).astype(jnp.float32)
    right = jnp.concatenate([d, e, d, f, d, e], axis=0)
    return dot(left.T.astype(jnp.bfloat16), right, precision=None)


NT = ((1,), (1,))
STOP = 1e-5
NEAR = 0.2
BOUND = 1e30
SHIFT = 4e-6


def step_inverse(low, inverse):
    mid = low.shape[0] // 2
    inverse_top, inverse_low = inverse[:mid, :mid], inverse[...]
    inverse[:mid, :mid] = inverse_top - dot3(low[:mid, :mid], inverse_top)
    inverse[mid:, :] = inverse_low[mid:] - dot3(low[mid:], inverse_low)


def opening_kernel(coeffs_ref, squares_ref, upper, square):
    coeffs = coeffs_ref[...]
    mid = coeffs.shape[1] // 2
    value = outer(coeffs, coeffs)
    upper[...] = value + jnp.where(diagonal(value), squares_ref[...], 0.0)
    square[:mid, :] = dot(upper[:mid, :], upper[...])
    square[mid:, :mid] = jnp.zeros((mid, mid), jnp.float32)
    square[mid:, mid:] = dot(upper[mid:, :], upper[:, mid:])


def opening(coeffs, squares):
    modes = coeffs.shape[1]
    spec = pl.BlockSpec(memory_space=pltpu.VMEM)
    shape = jax.ShapeDtypeStruct((modes, modes), jnp.float32)
    return pl.pallas_call(
        opening_kernel, out_shape=(shape, shape), in_specs=[spec] * 2, out_specs=(spec, spec),
        compiler_params=pltpu.CompilerParams(vmem_limit_bytes=VMEM),
        cost_estimate=pl.CostEstimate(
            flops=12 * modes**3, bytes_accessed=8 * modes**2, transcendentals=0
        ),
    )(coeffs, squares)


def pieces_kernel(basis_hbm, top, low, held, loaded):
    chunk = held.shape[1]
    count = basis_hbm.shape[0] // chunk
    copies = [
        pltpu.make_async_copy(
            basis_hbm.at[pl.ds(index * chunk, chunk), :], held.at[index % 2], loaded.at[index % 2]
        )
        for index in range(count)
    ]
    copies[0].start()
    for index in range(count):
        if index + 1 < count:
            copies[index + 1].start()
        copies[index].wait()
        here = pl.ds(index * chunk, chunk)
        top[here, :], low[here, :] = split(held[index % 2], 2)


def basis_pieces(old_basis):
    rows, modes = old_basis.shape
    chunk = chunk_of(rows)
    spec = pl.BlockSpec(memory_space=pltpu.VMEM)
    shape = jax.ShapeDtypeStruct((rows, modes), jnp.bfloat16)
    return pl.pallas_call(
        pieces_kernel, out_shape=(shape, shape),
        in_specs=[pl.BlockSpec(memory_space=pl.ANY)], out_specs=(spec, spec),
        scratch_shapes=[
            pltpu.VMEM((2, chunk, modes), jnp.float32), pltpu.SemaphoreType.DMA((2,))
        ],
        compiler_params=pltpu.CompilerParams(vmem_limit_bytes=VMEM),
        cost_estimate=pl.CostEstimate(
            flops=1000 * rows * modes, bytes_accessed=8 * rows * modes, transcendentals=0
        ),
    )(old_basis)


def deal_kernel(name, snaps_hbm, *refs):
    blocks, done = refs[:-1], refs[-1]
    cells = blocks[0].shape[1]
    index = lax.axis_index(name)
    copies = []
    for mask, block in enumerate(blocks):
        start = pl.multiple_of(jnp.bitwise_xor(index, mask) * cells, LANES)
        copies.append(
            pltpu.make_async_copy(snaps_hbm.at[:, pl.ds(start, cells)], block, done.at[mask])
        )
        copies[-1].start()
    for copy in copies:
        copy.wait()


def deal(snapshots, name):
    count = lax.axis_size(name)
    rows, cells = snapshots.shape[0], snapshots.shape[1] // count
    spec = pl.BlockSpec(memory_space=pltpu.VMEM)
    return pl.pallas_call(
        functools.partial(deal_kernel, name),
        out_shape=[jax.ShapeDtypeStruct((rows, cells), jnp.float32)] * count,
        in_specs=[pl.BlockSpec(memory_space=pl.ANY)], out_specs=[spec] * count,
        scratch_shapes=[pltpu.SemaphoreType.DMA((count,))],
        compiler_params=pltpu.CompilerParams(vmem_limit_bytes=VMEM),
    )(snapshots)


def coeffs_kernel(name, weight, count, *refs):
    top_ref, low_ref, out_ref, snaps_ref = refs[count:]
    if count == 1:
        snaps_ref[...] = refs[0][...]
    else:
        rows = refs[0].shape[0]
        index = lax.axis_index(name)
        for mask in range(count):
            start = pl.multiple_of(jnp.bitwise_xor(index, mask) * rows, rows)
            snaps_ref[pl.ds(start, rows), :] = refs[mask][...]
    snaps = snaps_ref.shape[0]
    top, low = split(snaps_ref[...], 2)
    value = dot(jnp.concatenate([top, low], axis=0), top_ref[...], precision=None)
    value = value[:snaps] + (value[snaps:] + dot(top, low_ref[...], precision=None))
    out_ref[...] = value * weight


def local_coeffs(blocks, basis_top, basis_low, weight):
    count = len(blocks)
    rows, modes = basis_top.shape
    snaps = count * blocks[0].shape[0]
    spec = pl.BlockSpec(memory_space=pltpu.VMEM)
    return pl.pallas_call(
        functools.partial(coeffs_kernel, AXES[0], weight, count),
        out_shape=(
            jax.ShapeDtypeStruct((snaps, modes), jnp.float32),
            jax.ShapeDtypeStruct((snaps, rows), jnp.float32),
        ),
        in_specs=[spec] * (count + 2), out_specs=(spec, spec),
        compiler_params=pltpu.CompilerParams(vmem_limit_bytes=VMEM),
    )(*blocks, basis_top, basis_low)


def rotation(coeffs_ref, gram_ref, upper, square_ref, inverse, second, work):
    coeffs = coeffs_ref[...]
    mid = coeffs.shape[1] // 2
    square = square_ref

    def first_gram():
        second[...] = square_ref[...] + outer(coeffs, dot(gram_ref[...], coeffs))

    first_gram()

    def far(carry):
        return jnp.logical_not(carry[1] < NEAR) & (carry[0] < 8)

    def factor_pass(carry):
        count, _, fresh = carry
        factor_inverse(second, work)

        @pl.when(fresh == 1)
        def _():
            inverse[...] = second[...]

        @pl.when(fresh == 0)
        def _():
            inverse[...] = dot(second[...], inverse[...])

        second[:mid, :] = dot(inverse[:mid, :mid], upper[:mid, :])
        second[mid:, :] = dot(inverse[mid:, :], upper[...])
        part = dot3(inverse[...], coeffs, NT)
        side = dot3(part, gram_ref[...])
        stacked = second[...]
        gram_low = dot3(stacked[mid:], stacked, NT) + dot3(side[mid:], part, NT)
        gram_top = dot3(stacked[:mid], stacked[:mid], NT) + dot3(side[:mid], part[:mid], NT)
        second[:mid, :mid] = gram_top
        second[mid:, :] = gram_low
        second[:mid, mid:] = gram_low[:, :mid].T
        rest = second[...] - jnp.where(diagonal(square), 1.0, 0.0)
        size = jnp.sum(rest * rest)
        failed = jnp.logical_not(size < BOUND)

        @pl.when(failed)
        def _():
            first_gram()
            ends = jnp.where(diagonal(square), second[...], 0.0)
            second[...] = second[...] + jnp.where(diagonal(square), SHIFT * jnp.max(ends), 0.0)

        return count + 1, size, failed.astype(jnp.int32)

    _, size, _ = lax.while_loop(far, factor_pass, (jnp.int32(0), jnp.float32(BOUND), jnp.int32(1)))

    second[...] = second[...] - jnp.where(diagonal(square), 1.0, 0.0)

    def more(carry):
        return (carry[0] >= STOP) & (carry[1] < 16)

    def newton(carry):
        rest = second[...]
        low = half(rest)
        step_inverse(low, inverse)
        mixed = dot3(low, rest)
        rest = dot3(low + mixed, low, NT) - mixed - mixed.T
        second[...] = rest
        return jnp.sum(rest * rest), carry[1] + 1

    lax.while_loop(more, newton, (size, jnp.int32(0)))
    step_inverse(half(second[...]), inverse)


def update_kernel(
    coeffs_ref, gram_ref, squares_ref, upper, square_ref, snaps_ref, top_ref, low_ref, out_hbm,
    inverse, second, work, out, stored,
):
    rows, modes = top_ref.shape
    mid = modes // 2
    rotation(coeffs_ref, gram_ref, upper, square_ref, inverse, second, work)
    final = inverse[...]
    turn_top, turn_low = split(final * squares_ref[...], 2)
    across_top, across_low = split(dot(final, coeffs_ref[...], NT).T, 2)
    across = jnp.concatenate([across_top, across_low, across_top], axis=0)
    chunk = chunk_of(rows)
    copies = []
    for start in range(0, rows, chunk):
        here = pl.ds(start, chunk)
        snaps_top, snaps_low = split(snaps_ref[:, pl.ds(start, chunk)], 2)
        mixed = jnp.concatenate([snaps_top, snaps_top, snaps_low], axis=0).astype(jnp.float32)
        base = dot(mixed.T.astype(jnp.bfloat16), across, precision=None)
        top, low = top_ref[here, :], low_ref[here, :]
        for cols, depth in ((slice(0, mid), mid), (slice(mid, modes), modes)):
            value = base[:, cols]
            for a, b in ((low, turn_top), (top, turn_low), (top, turn_top)):
                value = value + dot(a[:, :depth], b[cols, :depth], NT, None)
            out[here, cols] = value.astype(out.dtype)
        copies.append(pltpu.make_async_copy(out.at[here, :], out_hbm.at[here, :], stored.at[start // chunk]))
        copies[-1].start()
    for copy in copies:
        copy.wait()


def chunk_of(rows):
    for chunk in (640, 512, 384, 256, 128):
        if rows % chunk == 0:
            return chunk
    return rows


def updated_basis(coeffs, gram_res, squares, upper, square, snap_rows, basis_top, basis_low):
    rows, modes = basis_top.shape
    whole = pltpu.VMEM((modes, modes), jnp.float32)
    spec = pl.BlockSpec(memory_space=pltpu.VMEM)
    far = pl.BlockSpec(memory_space=pl.ANY)
    return pl.pallas_call(
        update_kernel,
        out_shape=jax.ShapeDtypeStruct((rows, modes), jnp.bfloat16),
        in_specs=[spec] * 8,
        out_specs=far,
        scratch_shapes=[
            whole, whole, pltpu.VMEM((BLOCK, BLOCK), jnp.float32),
            pltpu.VMEM((rows, modes), jnp.bfloat16), pltpu.SemaphoreType.DMA((rows // chunk_of(rows),)),
        ],
        compiler_params=pltpu.CompilerParams(vmem_limit_bytes=VMEM),
    )(coeffs, gram_res, squares, upper, square, snap_rows, basis_top, basis_low)


HIGH = lax.Precision.HIGH


def mat(left, right, contract, precision=HIGH):
    return lax.dot_general(
        left, right, (contract, ((), ())), precision=precision, preferred_element_type=jnp.float32
    )


AXES = ("tile", "slab")


def exchange(part, mask):
    count = lax.axis_size(AXES[0]) * lax.axis_size(AXES[1])
    return lax.ppermute(part, AXES, [(i, i ^ mask) for i in range(count)])


def sum_rounds():
    count = lax.axis_size(AXES[0]) * lax.axis_size(AXES[1])
    rounds, bit = [], 2
    while bit < count:
        rounds.append([bit, 2 * bit, 3 * bit] if 2 * bit < count else [bit])
        bit *= 4
    return rounds


def sum_round(part, masks):
    others = [exchange(part, mask) for mask in masks]
    if len(others) == 1:
        return part + others[0]
    return (part + others[0]) + (others[1] + others[2])


def sum_all(part):
    part = part + exchange(part, 1)
    for masks in sum_rounds():
        part = sum_round(part, masks)
    return part


def sum_all_halved(part):
    half_rows = part.shape[0] // 2
    first = lax.axis_index(AXES[1]) % 2 == 0
    top, low = part[:half_rows], part[half_rows:]
    kept = jnp.where(first, top, low) + exchange(jnp.where(first, low, top), 1)
    for masks in sum_rounds():
        kept = sum_round(kept, masks)
    other = exchange(kept, 1)
    return jnp.concatenate([jnp.where(first, kept, other), jnp.where(first, other, kept)], axis=0)


def exchange_rows(snapshots):
    name = AXES[0]
    count = lax.axis_size(name)
    if count > 8 or count & (count - 1) or snapshots.shape[0] % 8:
        return [lax.all_to_all(snapshots, name, split_axis=1, concat_axis=0, tiled=True)]
    blocks = deal(snapshots, name)
    return [
        lax.ppermute(block, name, [(i, i ^ mask) for i in range(count)]) if mask else block
        for mask, block in enumerate(blocks)
    ]


def local(snapshots, old_basis, sing_values):
    basis_top, basis_low = basis_pieces(old_basis)
    blocks = exchange_rows(snapshots)
    cell_count = old_basis.shape[0] * lax.axis_size("tile") * lax.axis_size("slab")
    weight_cell = 1.0 / cell_count
    part, snap_rows = local_coeffs(blocks, basis_top, basis_low, weight_cell)
    coeffs = sum_all_halved(part)
    resid = snap_rows - mat(coeffs, old_basis, ((1,), (1,)))
    gram_part = mat(resid, resid, ((1,), (1,))) * weight_cell
    squares = (sing_values * sing_values)[None, :]
    gram_res = sum_all(gram_part)
    upper, square = opening(lax.optimization_barrier((coeffs, gram_part))[0], squares)
    return updated_basis(
        coeffs, gram_res, squares, upper, square, snap_rows, basis_top, basis_low
    )


def solution(mesh):
    placed = (P("tile", "slab"), P(("slab", "tile"), None), P())
    return jax.shard_map(
        local, mesh=mesh, in_specs=placed, out_specs=P(("slab", "tile"), None), check_vma=False
    )
```

```python
import functools

import jax
import jax.numpy as jnp
from jax import lax
from jax.experimental import pallas as pl
from jax.experimental.pallas import tpu as pltpu
from jax.sharding import PartitionSpec as P

HIGHEST = lax.Precision.HIGHEST
BLOCK = 128
LANES = 128
VMEM = 28 * 1024 * 1024


def dot(left, right, contract=((1,), (0,)), precision=HIGHEST):
    return lax.dot_general(
        left, right, (contract, ((), ())), precision=precision, preferred_element_type=jnp.float32
    )


def spread(value, row):
    return jnp.broadcast_to(value[row : row + 1, :], value.shape)


def lane_spread(value, lane):
    return jnp.broadcast_to(value[:, lane : lane + 1], value.shape)


def total(terms):
    while len(terms) > 1:
        terms = [a + b for a, b in zip(terms[::2], terms[1::2])] + terms[len(terms) // 2 * 2 :]
    return terms[0]


def factor_block(work):
    size = work.shape[0]
    lanes = lax.broadcasted_iota(jnp.int32, (8, size), 1)
    subs = lax.broadcasted_iota(jnp.int32, (8, size), 0)
    first = work[pl.ds(0, 8), :]
    cols = [lane_spread(first, j) for j in range(8)]
    for step in range(size // 8):
        base = 8 * step
        inside = (lanes >= base) & (lanes < base + 8)
        last = step + 1 == size // 8
        below = {
            other: work[pl.ds(8 * other, 8), :] for other in range(step + 1, size // 8)
        }
        beside = {
            other: [lane_spread(rows, base + j) for j in range(8)] for other, rows in below.items()
        }
        ratio, recip = {}, []
        for j in range(8):
            pivot = spread(cols[j], j)
            pivots = pivot if j == 0 else jnp.where(subs == j, pivot, pivots)
            recip.append(1.0 / pivot)
            for k in range(j + 1, 8):
                ratio[j, k] = spread(cols[j], k) * recip[j]
                cols[k] = cols[k] - cols[j] * ratio[j, k]
        if not last:
            near = list(beside[step + 1])
            for j in range(8):
                for k in range(j + 1, 8):
                    near[k] = near[k] - near[j] * ratio[j, k]
            own = [lane_spread(below[step + 1], base + 8 + i) for i in range(8)]
            shares = [near[j] * recip[j] for j in range(8)]
            own = [
                own[i] - total([near[j] * spread(shares[j], i) for j in range(8)]) for i in range(8)
            ]
        row = work[pl.ds(base, 8), :]
        row = jnp.where(inside, jnp.where(lanes - base == subs, 1.0, 0.0), row)
        solved = []
        for j in range(8):
            solved.append(spread(row, j) * recip[j])
            if j < 7:
                row = row - jnp.where(subs > j, cols[j], 0.0) * solved[j]
        work[pl.ds(base, 8), :] = row * lax.rsqrt(pivots)
        for j in reversed(range(7)):
            solved[j] = solved[j] - total([ratio[j, k] * solved[k] for k in range(j + 1, 8)])
        for other, rows in below.items():
            work[pl.ds(8 * other, 8), :] = jnp.where(inside, 0.0, rows) - total(
                [beside[other][j] * solved[j] for j in range(8)]
            )
        if not last:
            cols = own


def tril(value):
    rows = lax.broadcasted_iota(jnp.int32, value.shape, 0)
    return jnp.where(lax.broadcasted_iota(jnp.int32, value.shape, 1) <= rows, value, 0.0)


def split(value, parts):
    pieces = []
    for _ in range(parts):
        pieces.append(value.astype(jnp.bfloat16))
        value = value - pieces[-1].astype(jnp.float32)
    return pieces


def block_dot(left, right):
    a, b, c = split(left, 3)
    d, e, f = split(right, 3)
    both = jnp.concatenate([d, e], axis=0)
    value = dot(jnp.concatenate([a, c], axis=1), jnp.concatenate([f, d], axis=0), precision=None)
    value = value + dot(jnp.concatenate([b, b], axis=1), both, precision=None)
    return value + dot(jnp.concatenate([a, a], axis=1), both, precision=None)


def factor_inverse(gram, work):
    size = gram.shape[0]
    count = size // BLOCK

    def step(index, carry):
        start = pl.multiple_of(index * BLOCK, BLOCK)
        here = pl.ds(start, BLOCK)
        work[...] = gram[here, here]
        factor_block(work)
        inverse = tril(work[...])
        gram[here, here] = jnp.eye(BLOCK, dtype=jnp.float32)
        for block in range(count):

            @pl.when(index == block)
            def _():
                low = BLOCK * block
                high = low + BLOCK
                row = block_dot(inverse, gram[low:high, :])
                gram[low:high, :] = row
                if high < size:
                    gram[high:, low:high] = jnp.zeros((size - high, BLOCK), jnp.float32)
                    gram[high:, :] = gram[high:, :] - block_dot(row[:, high:].T, row)

        return carry

    lax.fori_loop(0, count, step, 0)
    gram[...] = tril(gram[...])


def diagonal(value):
    rows = lax.broadcasted_iota(jnp.int32, value.shape, 0)
    cols = lax.broadcasted_iota(jnp.int32, value.shape, 1)
    return rows == cols


def half(value, offset=0):
    rows = lax.broadcasted_iota(jnp.int32, value.shape, 0) + offset
    cols = lax.broadcasted_iota(jnp.int32, value.shape, 1)
    return jnp.where(rows > cols, value, jnp.where(rows == cols, 0.5 * value, 0.0))


def dot3(left, right, contract=((1,), (0,))):
    left_top, left_low = split(left, 2)
    right_top, right_low = split(right, 2)
    small = dot(left_low, right_top, contract, None) + dot(left_top, right_low, contract, None)
    return dot(left_top, right_top, contract, None) + small


def outer(left, right, exact=True):
    a, b, c = split(left, 3)
    d, e, f = split(right, 3)
    lefts, rights = ([a, a, b, a, c, b], [d, e, d, f, d, e]) if exact else ([a, a, b], [d, e, d])
    left = jnp.concatenate(lefts, axis=0).astype(jnp.float32)
    return dot(left.T.astype(jnp.bfloat16), jnp.concatenate(rights, axis=0), precision=None)


NT = ((1,), (1,))
STOP = 1e-5
NEAR = 0.2
BOUND = 1e30
SHIFT = 4e-6


def step_inverse(low, inverse):
    mid = low.shape[0] // 2
    inverse_top, inverse_low = inverse[:mid, :mid], inverse[...]
    inverse[:mid, :mid] = inverse_top - dot3(low[:mid, :mid], inverse_top)
    inverse[mid:, :] = inverse_low[mid:] - dot3(low[mid:], inverse_low)


def opening_kernel(coeffs_ref, squares_ref, upper, square):
    coeffs = coeffs_ref[...]
    mid = coeffs.shape[1] // 2
    value = outer(coeffs, coeffs)
    upper[...] = value + jnp.where(diagonal(value), squares_ref[...], 0.0)
    square[:mid, :] = dot(upper[:mid, :], upper[...])
    square[mid:, :mid] = jnp.zeros((mid, mid), jnp.float32)
    square[mid:, mid:] = dot(upper[mid:, :], upper[:, mid:])


def opening(coeffs, squares):
    modes = coeffs.shape[1]
    spec = pl.BlockSpec(memory_space=pltpu.VMEM)
    shape = jax.ShapeDtypeStruct((modes, modes), jnp.float32)
    return pl.pallas_call(
        opening_kernel, out_shape=(shape, shape), in_specs=[spec] * 2, out_specs=(spec, spec),
        compiler_params=pltpu.CompilerParams(vmem_limit_bytes=VMEM),
        cost_estimate=pl.CostEstimate(
            flops=12 * modes**3, bytes_accessed=8 * modes**2, transcendentals=0
        ),
    )(coeffs, squares)


def pieces_kernel(basis_hbm, top, low, held, loaded):
    chunk = held.shape[1]
    count = basis_hbm.shape[0] // chunk
    copies = [
        pltpu.make_async_copy(
            basis_hbm.at[pl.ds(index * chunk, chunk), :], held.at[index % 2], loaded.at[index % 2]
        )
        for index in range(count)
    ]
    copies[0].start()
    for index in range(count):
        if index + 1 < count:
            copies[index + 1].start()
        copies[index].wait()
        here = pl.ds(index * chunk, chunk)
        top[here, :], low[here, :] = split(held[index % 2], 2)


def basis_pieces(old_basis):
    rows, modes = old_basis.shape
    chunk = chunk_of(rows)
    spec = pl.BlockSpec(memory_space=pltpu.VMEM)
    shape = jax.ShapeDtypeStruct((rows, modes), jnp.bfloat16)
    return pl.pallas_call(
        pieces_kernel, out_shape=(shape, shape),
        in_specs=[pl.BlockSpec(memory_space=pltpu.HBM)], out_specs=(spec, spec),
        scratch_shapes=[
            pltpu.VMEM((2, chunk, modes), jnp.float32), pltpu.SemaphoreType.DMA((2,))
        ],
        compiler_params=pltpu.CompilerParams(vmem_limit_bytes=VMEM),
        cost_estimate=pl.CostEstimate(
            flops=1000 * rows * modes, bytes_accessed=8 * rows * modes, transcendentals=0
        ),
    )(old_basis)


def deal_kernel(name, snaps_ref, *blocks):
    cells = blocks[0].shape[1]
    index = lax.axis_index(name)
    for mask, block in enumerate(blocks):
        start = pl.multiple_of(jnp.bitwise_xor(index, mask) * cells, LANES)
        block[...] = snaps_ref[:, pl.ds(start, cells)]


def deal(snapshots, name):
    count = lax.axis_size(name)
    rows, cells = snapshots.shape[0], snapshots.shape[1] // count
    spec = pl.BlockSpec(memory_space=pltpu.VMEM)
    return pl.pallas_call(
        functools.partial(deal_kernel, name),
        out_shape=[jax.ShapeDtypeStruct((rows, cells), jnp.float32)] * count,
        in_specs=[spec], out_specs=[spec] * count,
        compiler_params=pltpu.CompilerParams(vmem_limit_bytes=VMEM),
    )(snapshots)


def coeffs_kernel(name, weight, count, *refs):
    top_ref, low_ref, out_ref, snaps_ref = refs[count:]
    if count == 1:
        snaps_ref[...] = refs[0][...]
    else:
        rows = refs[0].shape[0]
        index = lax.axis_index(name)
        for mask in range(count):
            start = pl.multiple_of(jnp.bitwise_xor(index, mask) * rows, rows)
            snaps_ref[pl.ds(start, rows), :] = refs[mask][...]
    snaps = snaps_ref.shape[0]
    top, low = split(snaps_ref[...], 2)
    value = dot(jnp.concatenate([top, low], axis=0), top_ref[...], precision=None)
    value = value[:snaps] + (value[snaps:] + dot(top, low_ref[...], precision=None))
    out_ref[...] = value * weight


def local_coeffs(blocks, basis_top, basis_low, weight):
    count = len(blocks)
    rows, modes = basis_top.shape
    snaps = count * blocks[0].shape[0]
    spec = pl.BlockSpec(memory_space=pltpu.VMEM)
    return pl.pallas_call(
        functools.partial(coeffs_kernel, AXES[0], weight, count),
        out_shape=(
            jax.ShapeDtypeStruct((snaps, modes), jnp.float32),
            jax.ShapeDtypeStruct((snaps, rows), jnp.float32),
        ),
        in_specs=[spec] * (count + 2), out_specs=(spec, spec),
        compiler_params=pltpu.CompilerParams(vmem_limit_bytes=VMEM),
    )(*blocks, basis_top, basis_low)


def rotation(coeffs_ref, gram_ref, upper, square_ref, inverse, second, work):
    coeffs = coeffs_ref[...]
    mid = coeffs.shape[1] // 2

    def first_gram():
        second[...] = square_ref[...] + outer(coeffs, dot(gram_ref[...], coeffs))

    first_gram()

    def far(carry):
        return jnp.logical_not(carry[1] < NEAR) & (carry[0] < 12)

    one = jnp.where(diagonal(square_ref), 1.0, 0.0)

    def mirror():
        second[:mid, mid:] = second[mid:, :mid].T

    def factor_pass(carry):
        count, _, fresh, shift = carry

        @pl.when(count > 0)
        def _():
            second[...] = second[...] + one

        factor_inverse(second, work)

        @pl.when(fresh == 1)
        def _():
            inverse[...] = second[...]

        @pl.when(fresh == 0)
        def _():
            inverse[...] = dot(second[...], inverse[...])

        part = dot3(coeffs, inverse[...], NT)
        side = dot3(gram_ref[...], part)
        extra = outer(side, part, False) - one
        second[:mid, :] = dot(inverse[:mid, :mid], upper[:mid, :])
        second[mid:, :] = dot(inverse[mid:, :], upper[...])
        stacked = second[...]
        rest_low = dot3(stacked[mid:], stacked, NT) + extra[mid:]
        rest_top = dot3(stacked[:mid], stacked[:mid], NT) + extra[:mid, :mid]
        second[:mid, :mid] = rest_top
        second[mid:, :] = rest_low
        size = (
            jnp.sum(rest_top * rest_top)
            + jnp.sum(rest_low[:, mid:] * rest_low[:, mid:])
            + 2.0 * jnp.sum(rest_low[:, :mid] * rest_low[:, :mid])
        )
        failed = jnp.logical_not(size < BOUND)

        @pl.when(failed)
        def _():
            first_gram()
            ends = one * second[...]
            second[...] = second[...] + (shift * jnp.max(ends) - 1.0) * one

        @pl.when(jnp.logical_not(failed) & (size >= STOP))
        def _():
            mirror()

        return count + 1, size, failed.astype(jnp.int32), jnp.where(failed, 8.0 * shift, shift)

    first = (jnp.int32(0), jnp.float32(BOUND), jnp.int32(1), jnp.float32(SHIFT))
    size = lax.while_loop(far, factor_pass, first)[1]

    def more(carry):
        return (carry[0] >= STOP) & (carry[1] < 16)

    def newton(carry):
        rest = second[...]
        low = half(rest)
        step_inverse(low, inverse)
        mixed = dot3(low, rest)
        rest = dot3(low + mixed, low, NT) - mixed - mixed.T
        second[...] = rest
        return jnp.sum(rest * rest), carry[1] + 1

    lax.while_loop(more, newton, (size, jnp.int32(0)))
    step_inverse(half(second[...]), inverse)


def update_kernel(
    coeffs_ref, gram_ref, squares_ref, upper, square_ref, snaps_ref, top_ref, low_ref, out_hbm,
    inverse, second, work, out, stored,
):
    rows, modes = top_ref.shape
    mid = modes // 2
    rotation(coeffs_ref, gram_ref, upper, square_ref, inverse, second, work)
    final = inverse[...]
    turn_top, turn_low = split(final * squares_ref[...], 2)
    across_top, across_low = split(dot(coeffs_ref[...], final, NT), 2)
    across = jnp.concatenate([across_top, across_low, across_top], axis=0)
    chunk = chunk_of(rows)
    copies = []
    for start in range(0, rows, chunk):
        here = pl.ds(start, chunk)
        snaps_top, snaps_low = split(snaps_ref[:, pl.ds(start, chunk)], 2)
        mixed = jnp.concatenate([snaps_top, snaps_top, snaps_low], axis=0).astype(jnp.float32)
        base = dot(mixed.T.astype(jnp.bfloat16), across, precision=None)
        top, low = top_ref[here, :], low_ref[here, :]
        for cols, depth in ((slice(0, mid), mid), (slice(mid, modes), modes)):
            value = base[:, cols]
            for a, b in ((low, turn_top), (top, turn_low), (top, turn_top)):
                value = value + dot(a[:, :depth], b[cols, :depth], NT, None)
            out[here, cols] = value.astype(out.dtype)
        copies.append(pltpu.make_async_copy(out.at[here, :], out_hbm.at[here, :], stored.at[start // chunk]))
        copies[-1].start()
    for copy in copies:
        copy.wait()


def chunk_of(rows):
    for chunk in (640, 512, 384, 256, 128):
        if rows % chunk == 0:
            return chunk
    return rows


def updated_basis(coeffs, gram_res, squares, upper, square, snap_rows, basis_top, basis_low):
    rows, modes = basis_top.shape
    whole = pltpu.VMEM((modes, modes), jnp.float32)
    spec = pl.BlockSpec(memory_space=pltpu.VMEM)
    far = pl.BlockSpec(memory_space=pl.ANY)
    return pl.pallas_call(
        update_kernel,
        out_shape=jax.ShapeDtypeStruct((rows, modes), jnp.bfloat16),
        in_specs=[spec] * 8,
        out_specs=far,
        scratch_shapes=[
            whole, whole, pltpu.VMEM((BLOCK, BLOCK), jnp.float32),
            pltpu.VMEM((rows, modes), jnp.bfloat16), pltpu.SemaphoreType.DMA((rows // chunk_of(rows),)),
        ],
        compiler_params=pltpu.CompilerParams(vmem_limit_bytes=VMEM),
    )(coeffs, gram_res, squares, upper, square, snap_rows, basis_top, basis_low)


HIGH = lax.Precision.HIGH


def mat(left, right, contract, precision=HIGH):
    return lax.dot_general(
        left, right, (contract, ((), ())), precision=precision, preferred_element_type=jnp.float32
    )


AXES = ("tile", "slab")


def exchange(part, mask):
    count = lax.axis_size(AXES[0]) * lax.axis_size(AXES[1])
    return lax.ppermute(part, AXES, [(i, i ^ mask) for i in range(count)])


def sum_rounds():
    count = lax.axis_size(AXES[0]) * lax.axis_size(AXES[1])
    rounds, bit = [], 2
    while bit < count:
        rounds.append([bit, 2 * bit, 3 * bit] if 2 * bit < count else [bit])
        bit *= 4
    return rounds


def sum_round(part, masks):
    others = [exchange(part, mask) for mask in masks]
    if len(others) == 1:
        return part + others[0]
    return (part + others[0]) + (others[1] + others[2])


def sum_all(part):
    part = part + exchange(part, 1)
    for masks in sum_rounds():
        part = sum_round(part, masks)
    return part


def sum_all_halved(part):
    half_rows = part.shape[0] // 2
    first = lax.axis_index(AXES[1]) % 2 == 0
    top, low = part[:half_rows], part[half_rows:]
    kept = jnp.where(first, top, low) + exchange(jnp.where(first, low, top), 1)
    for masks in sum_rounds():
        kept = sum_round(kept, masks)
    other = exchange(kept, 1)
    return jnp.concatenate([jnp.where(first, kept, other), jnp.where(first, other, kept)], axis=0)


def exchange_rows(snapshots):
    name = AXES[0]
    count = lax.axis_size(name)
    if count > 8 or count & (count - 1) or snapshots.shape[0] % 8 or snapshots.shape[1] % (count * LANES):
        return [lax.all_to_all(snapshots, name, split_axis=1, concat_axis=0, tiled=True)]
    blocks = list(deal(snapshots, name))
    return [
        lax.ppermute(block, name, [(i, i ^ mask) for i in range(count)]) if mask else block
        for mask, block in enumerate(blocks)
    ]


def local(snapshots, old_basis, sing_values):
    basis_top, basis_low = basis_pieces(old_basis)
    blocks = exchange_rows(snapshots)
    cell_count = old_basis.shape[0] * lax.axis_size("tile") * lax.axis_size("slab")
    weight_cell = 1.0 / cell_count
    part, snap_rows = local_coeffs(blocks, basis_top, basis_low, weight_cell)
    coeffs = sum_all_halved(part)
    resid = snap_rows - mat(coeffs, old_basis, ((1,), (1,)))
    gram_part = mat(resid, resid, ((1,), (1,))) * weight_cell
    squares = (sing_values * sing_values)[None, :]
    gram_res = sum_all(gram_part)
    upper, square = opening(lax.optimization_barrier((coeffs, gram_part))[0], squares)
    return updated_basis(
        coeffs, gram_res, squares, upper, square, snap_rows, basis_top, basis_low
    )


def solution(mesh):
    placed = (P("tile", "slab"), P(("slab", "tile"), None), P())
    return jax.shard_map(
        local, mesh=mesh, in_specs=placed, out_specs=P(("slab", "tile"), None), check_vma=False
    )
```

```python
import functools

import jax
import jax.numpy as jnp
from jax import lax
from jax.experimental import pallas as pl
from jax.experimental.pallas import tpu as pltpu
from jax.sharding import PartitionSpec as P

HIGHEST = lax.Precision.HIGHEST
BLOCK = 128
LANES = 128
VMEM = 28 * 1024 * 1024


def dot(left, right, contract=((1,), (0,)), precision=HIGHEST):
    return lax.dot_general(
        left, right, (contract, ((), ())), precision=precision, preferred_element_type=jnp.float32
    )


def spread(value, row):
    return jnp.broadcast_to(value[row : row + 1, :], value.shape)


def lane_spread(value, lane):
    return jnp.broadcast_to(value[:, lane : lane + 1], value.shape)


def total(terms):
    while len(terms) > 1:
        terms = [a + b for a, b in zip(terms[::2], terms[1::2])] + terms[len(terms) // 2 * 2 :]
    return terms[0]


def factor_block(work):
    size = work.shape[0]
    lanes = lax.broadcasted_iota(jnp.int32, (8, size), 1)
    subs = lax.broadcasted_iota(jnp.int32, (8, size), 0)
    first = work[pl.ds(0, 8), :]
    cols = [lane_spread(first, j) for j in range(8)]
    for step in range(size // 8):
        base = 8 * step
        inside = (lanes >= base) & (lanes < base + 8)
        last = step + 1 == size // 8
        below = {
            other: work[pl.ds(8 * other, 8), :] for other in range(step + 1, size // 8)
        }
        beside = {
            other: [lane_spread(rows, base + j) for j in range(8)] for other, rows in below.items()
        }
        ratio, recip = {}, []
        for j in range(8):
            pivot = spread(cols[j], j)
            pivots = pivot if j == 0 else jnp.where(subs == j, pivot, pivots)
            recip.append(1.0 / pivot)
            for k in range(j + 1, 8):
                ratio[j, k] = spread(cols[j], k) * recip[j]
                cols[k] = cols[k] - cols[j] * ratio[j, k]
        if not last:
            near = list(beside[step + 1])
            for j in range(8):
                for k in range(j + 1, 8):
                    near[k] = near[k] - near[j] * ratio[j, k]
            own = [lane_spread(below[step + 1], base + 8 + i) for i in range(8)]
            shares = [near[j] * recip[j] for j in range(8)]
            own = [
                own[i] - total([near[j] * spread(shares[j], i) for j in range(8)]) for i in range(8)
            ]
        row = work[pl.ds(base, 8), :]
        row = jnp.where(inside, jnp.where(lanes - base == subs, 1.0, 0.0), row)
        solved = []
        for j in range(8):
            solved.append(spread(row, j) * recip[j])
            if j < 7:
                row = row - jnp.where(subs > j, cols[j], 0.0) * solved[j]
        work[pl.ds(base, 8), :] = row * lax.rsqrt(pivots)
        for j in reversed(range(7)):
            solved[j] = solved[j] - total([ratio[j, k] * solved[k] for k in range(j + 1, 8)])
        for other, rows in below.items():
            work[pl.ds(8 * other, 8), :] = jnp.where(inside, 0.0, rows) - total(
                [beside[other][j] * solved[j] for j in range(8)]
            )
        if not last:
            cols = own


def tril(value):
    rows = lax.broadcasted_iota(jnp.int32, value.shape, 0)
    return jnp.where(lax.broadcasted_iota(jnp.int32, value.shape, 1) <= rows, value, 0.0)


def split(value, parts):
    pieces = []
    for _ in range(parts):
        pieces.append(value.astype(jnp.bfloat16))
        value = value - pieces[-1].astype(jnp.float32)
    return pieces


def block_dot(left, right):
    a, b, c = split(left, 3)
    d, e, f = split(right, 3)
    both = jnp.concatenate([d, e], axis=0)
    value = dot(jnp.concatenate([a, c], axis=1), jnp.concatenate([f, d], axis=0), precision=None)
    value = value + dot(jnp.concatenate([b, b], axis=1), both, precision=None)
    return value + dot(jnp.concatenate([a, a], axis=1), both, precision=None)


def factor_inverse(gram, work):
    size = gram.shape[0]
    count = size // BLOCK

    def step(index, carry):
        start = pl.multiple_of(index * BLOCK, BLOCK)
        here = pl.ds(start, BLOCK)
        work[...] = gram[here, here]
        factor_block(work)
        inverse = tril(work[...])
        gram[here, here] = jnp.eye(BLOCK, dtype=jnp.float32)
        for block in range(count):

            @pl.when(index == block)
            def _():
                low = BLOCK * block
                high = low + BLOCK
                row = block_dot(inverse, gram[low:high, :])
                gram[low:high, :] = row
                if high < size:
                    gram[high:, low:high] = jnp.zeros((size - high, BLOCK), jnp.float32)
                    gram[high:, :] = gram[high:, :] - block_dot(row[:, high:].T, row)

        return carry

    lax.fori_loop(0, count, step, 0)
    gram[...] = tril(gram[...])


def diagonal(value):
    rows = lax.broadcasted_iota(jnp.int32, value.shape, 0)
    cols = lax.broadcasted_iota(jnp.int32, value.shape, 1)
    return rows == cols


def half(value, offset=0):
    rows = lax.broadcasted_iota(jnp.int32, value.shape, 0) + offset
    cols = lax.broadcasted_iota(jnp.int32, value.shape, 1)
    return jnp.where(rows > cols, value, jnp.where(rows == cols, 0.5 * value, 0.0))


def dot3(left, right, contract=((1,), (0,))):
    left_top, left_low = split(left, 2)
    right_top, right_low = split(right, 2)
    small = dot(left_low, right_top, contract, None) + dot(left_top, right_low, contract, None)
    return dot(left_top, right_top, contract, None) + small


def outer(left, right, exact=True):
    a, b, c = split(left, 3)
    d, e, f = split(right, 3)
    lefts, rights = ([a, a, b, a, c, b], [d, e, d, f, d, e]) if exact else ([a, a, b], [d, e, d])
    left = jnp.concatenate(lefts, axis=0).astype(jnp.float32)
    return dot(left.T.astype(jnp.bfloat16), jnp.concatenate(rights, axis=0), precision=None)


NT = ((1,), (1,))
STOP = 1e-5
NEAR = 0.2
BOUND = 1e30
SHIFT = 4e-6


def step_inverse(low, inverse):
    mid = low.shape[0] // 2
    inverse_top, inverse_low = inverse[:mid, :mid], inverse[...]
    inverse[:mid, :mid] = inverse_top - dot3(low[:mid, :mid], inverse_top)
    inverse[mid:, :] = inverse_low[mid:] - dot3(low[mid:], inverse_low)


def opening_kernel(coeffs_ref, squares_ref, upper, square):
    coeffs = coeffs_ref[...]
    mid = coeffs.shape[1] // 2
    value = outer(coeffs, coeffs)
    upper[...] = value + jnp.where(diagonal(value), squares_ref[...], 0.0)
    square[:mid, :] = dot(upper[:mid, :], upper[...])
    square[mid:, :mid] = jnp.zeros((mid, mid), jnp.float32)
    square[mid:, mid:] = dot(upper[mid:, :], upper[:, mid:])


def opening(coeffs, squares):
    modes = coeffs.shape[1]
    spec = pl.BlockSpec(memory_space=pltpu.VMEM)
    shape = jax.ShapeDtypeStruct((modes, modes), jnp.float32)
    return pl.pallas_call(
        opening_kernel, out_shape=(shape, shape), in_specs=[spec] * 2, out_specs=(spec, spec),
        compiler_params=pltpu.CompilerParams(vmem_limit_bytes=VMEM),
        cost_estimate=pl.CostEstimate(
            flops=12 * modes**3, bytes_accessed=8 * modes**2, transcendentals=0
        ),
    )(coeffs, squares)


def pieces_kernel(basis_hbm, top, low, held, loaded):
    chunk = held.shape[1]
    count = basis_hbm.shape[0] // chunk
    copies = [
        pltpu.make_async_copy(
            basis_hbm.at[pl.ds(index * chunk, chunk), :], held.at[index % 2], loaded.at[index % 2]
        )
        for index in range(count)
    ]
    copies[0].start()
    for index in range(count):
        if index + 1 < count:
            copies[index + 1].start()
        copies[index].wait()
        here = pl.ds(index * chunk, chunk)
        top[here, :], low[here, :] = split(held[index % 2], 2)


def basis_pieces(old_basis):
    rows, modes = old_basis.shape
    chunk = chunk_of(rows)
    spec = pl.BlockSpec(memory_space=pltpu.VMEM)
    shape = jax.ShapeDtypeStruct((rows, modes), jnp.bfloat16)
    return pl.pallas_call(
        pieces_kernel, out_shape=(shape, shape),
        in_specs=[pl.BlockSpec(memory_space=pltpu.HBM)], out_specs=(spec, spec),
        scratch_shapes=[
            pltpu.VMEM((2, chunk, modes), jnp.float32), pltpu.SemaphoreType.DMA((2,))
        ],
        compiler_params=pltpu.CompilerParams(vmem_limit_bytes=VMEM),
        cost_estimate=pl.CostEstimate(
            flops=1000 * rows * modes, bytes_accessed=8 * rows * modes, transcendentals=0
        ),
    )(old_basis)


def deal_kernel(name, snaps_ref, *blocks):
    cells = blocks[0].shape[1]
    index = lax.axis_index(name)
    for mask, block in enumerate(blocks):
        start = pl.multiple_of(jnp.bitwise_xor(index, mask) * cells, LANES)
        block[...] = snaps_ref[:, pl.ds(start, cells)]


def deal(snapshots, name):
    count = lax.axis_size(name)
    rows, cells = snapshots.shape[0], snapshots.shape[1] // count
    spec = pl.BlockSpec(memory_space=pltpu.VMEM)
    return pl.pallas_call(
        functools.partial(deal_kernel, name),
        out_shape=[jax.ShapeDtypeStruct((rows, cells), jnp.float32)] * count,
        in_specs=[spec], out_specs=[spec] * count,
        compiler_params=pltpu.CompilerParams(vmem_limit_bytes=VMEM),
    )(snapshots)


def coeffs_kernel(name, weight, count, *refs):
    top_ref, low_ref, out_ref, snaps_ref = refs[count:]
    if count == 1:
        snaps_ref[...] = refs[0][...]
    else:
        rows = refs[0].shape[0]
        index = lax.axis_index(name)
        for mask in range(count):
            start = pl.multiple_of(jnp.bitwise_xor(index, mask) * rows, rows)
            snaps_ref[pl.ds(start, rows), :] = refs[mask][...]
    snaps = snaps_ref.shape[0]
    top, low = split(snaps_ref[...], 2)
    value = dot(jnp.concatenate([top, low], axis=0), top_ref[...], precision=None)
    value = value[:snaps] + (value[snaps:] + dot(top, low_ref[...], precision=None))
    out_ref[...] = value * weight


def local_coeffs(blocks, basis_top, basis_low, weight):
    count = len(blocks)
    rows, modes = basis_top.shape
    snaps = count * blocks[0].shape[0]
    spec = pl.BlockSpec(memory_space=pltpu.VMEM)
    return pl.pallas_call(
        functools.partial(coeffs_kernel, AXES[0], weight, count),
        out_shape=(
            jax.ShapeDtypeStruct((snaps, modes), jnp.float32),
            jax.ShapeDtypeStruct((snaps, rows), jnp.float32),
        ),
        in_specs=[spec] * (count + 2), out_specs=(spec, spec),
        compiler_params=pltpu.CompilerParams(vmem_limit_bytes=VMEM),
    )(*blocks, basis_top, basis_low)


def residual_kernel(weight, coeffs_ref, snaps_ref, top_ref, low_ref, out_ref):
    snaps = snaps_ref.shape[0]
    top, low = split(coeffs_ref[...], 2)
    value = dot(jnp.concatenate([top, low], axis=0), top_ref[...], NT, None)
    value = value[:snaps] + (value[snaps:] + dot(top, low_ref[...], NT, None))
    top, low = split(snaps_ref[...] - value, 2)
    value = dot(jnp.concatenate([top, low], axis=0), top, NT, None)
    out_ref[...] = (value[:snaps] + (value[snaps:] + value[snaps:].T)) * weight


def residual_gram(coeffs, snap_rows, basis_top, basis_low, weight):
    snaps = coeffs.shape[0]
    spec = pl.BlockSpec(memory_space=pltpu.VMEM)
    return pl.pallas_call(
        functools.partial(residual_kernel, weight),
        out_shape=jax.ShapeDtypeStruct((snaps, snaps), jnp.float32),
        in_specs=[spec] * 4, out_specs=spec,
        compiler_params=pltpu.CompilerParams(vmem_limit_bytes=VMEM),
    )(coeffs, snap_rows, basis_top, basis_low)


def rotation(coeffs_ref, gram_ref, upper, square_ref, inverse, second, work):
    coeffs = coeffs_ref[...]
    mid = coeffs.shape[1] // 2

    def first_gram():
        second[...] = square_ref[...] + outer(coeffs, dot(gram_ref[...], coeffs))

    first_gram()

    def far(carry):
        return jnp.logical_not(carry[1] < NEAR) & (carry[0] < 12)

    one = jnp.where(diagonal(square_ref), 1.0, 0.0)

    def mirror():
        second[:mid, mid:] = second[mid:, :mid].T

    def factor_pass(carry):
        count, _, fresh, shift = carry

        @pl.when(count > 0)
        def _():
            second[...] = second[...] + one

        factor_inverse(second, work)

        @pl.when(fresh == 1)
        def _():
            inverse[...] = second[...]

        @pl.when(fresh == 0)
        def _():
            inverse[...] = dot(second[...], inverse[...])

        part = dot3(coeffs, inverse[...], NT)
        side = dot3(gram_ref[...], part)
        extra = outer(side, part, False) - one
        second[:mid, :] = dot(inverse[:mid, :mid], upper[:mid, :])
        second[mid:, :] = dot(inverse[mid:, :], upper[...])
        stacked = second[...]
        rest_low = dot3(stacked[mid:], stacked, NT) + extra[mid:]
        rest_top = dot3(stacked[:mid], stacked[:mid], NT) + extra[:mid, :mid]
        second[:mid, :mid] = rest_top
        second[mid:, :] = rest_low
        size = (
            jnp.sum(rest_top * rest_top)
            + jnp.sum(rest_low[:, mid:] * rest_low[:, mid:])
            + 2.0 * jnp.sum(rest_low[:, :mid] * rest_low[:, :mid])
        )
        failed = jnp.logical_not(size < BOUND)

        @pl.when(failed)
        def _():
            first_gram()
            ends = one * second[...]
            second[...] = second[...] + (shift * jnp.max(ends) - 1.0) * one

        @pl.when(jnp.logical_not(failed) & (size >= STOP))
        def _():
            mirror()

        return count + 1, size, failed.astype(jnp.int32), jnp.where(failed, 8.0 * shift, shift)

    first = (jnp.int32(0), jnp.float32(BOUND), jnp.int32(1), jnp.float32(SHIFT))
    size = lax.while_loop(far, factor_pass, first)[1]

    def more(carry):
        return (carry[0] >= STOP) & (carry[1] < 16)

    def newton(carry):
        rest = second[...]
        low = half(rest)
        step_inverse(low, inverse)
        mixed = dot3(low, rest)
        rest = dot3(low + mixed, low, NT) - mixed - mixed.T
        second[...] = rest
        return jnp.sum(rest * rest), carry[1] + 1

    lax.while_loop(more, newton, (size, jnp.int32(0)))
    step_inverse(half(second[...]), inverse)


def update_kernel(
    coeffs_ref, gram_ref, squares_ref, upper, square_ref, snaps_ref, top_ref, low_ref, out_hbm,
    inverse, second, work, out, stored,
):
    rows, modes = top_ref.shape
    mid = modes // 2
    rotation(coeffs_ref, gram_ref, upper, square_ref, inverse, second, work)
    final = inverse[...]
    turn_top, turn_low = split(final * squares_ref[...], 2)
    across_top, across_low = split(dot(coeffs_ref[...], final, NT), 2)
    across = jnp.concatenate([across_top, across_low, across_top], axis=0)
    chunk = chunk_of(rows)
    copies = []
    for start in range(0, rows, chunk):
        here = pl.ds(start, chunk)
        snaps_top, snaps_low = split(snaps_ref[:, pl.ds(start, chunk)], 2)
        mixed = jnp.concatenate([snaps_top, snaps_top, snaps_low], axis=0).astype(jnp.float32)
        base = dot(mixed.T.astype(jnp.bfloat16), across, precision=None)
        top, low = top_ref[here, :], low_ref[here, :]
        for cols, depth in ((slice(0, mid), mid), (slice(mid, modes), modes)):
            value = base[:, cols]
            for a, b in ((low, turn_top), (top, turn_low), (top, turn_top)):
                value = value + dot(a[:, :depth], b[cols, :depth], NT, None)
            out[here, cols] = value.astype(out.dtype)
        copies.append(pltpu.make_async_copy(out.at[here, :], out_hbm.at[here, :], stored.at[start // chunk]))
        copies[-1].start()
    for copy in copies:
        copy.wait()


def chunk_of(rows):
    for chunk in (640, 512, 384, 256, 128):
        if rows % chunk == 0:
            return chunk
    return rows


def updated_basis(coeffs, gram_res, squares, upper, square, snap_rows, basis_top, basis_low):
    rows, modes = basis_top.shape
    whole = pltpu.VMEM((modes, modes), jnp.float32)
    spec = pl.BlockSpec(memory_space=pltpu.VMEM)
    far = pl.BlockSpec(memory_space=pl.ANY)
    return pl.pallas_call(
        update_kernel,
        out_shape=jax.ShapeDtypeStruct((rows, modes), jnp.bfloat16),
        in_specs=[spec] * 8,
        out_specs=far,
        scratch_shapes=[
            whole, whole, pltpu.VMEM((BLOCK, BLOCK), jnp.float32),
            pltpu.VMEM((rows, modes), jnp.bfloat16), pltpu.SemaphoreType.DMA((rows // chunk_of(rows),)),
        ],
        compiler_params=pltpu.CompilerParams(vmem_limit_bytes=VMEM),
    )(coeffs, gram_res, squares, upper, square, snap_rows, basis_top, basis_low)


AXES = ("tile", "slab")


def exchange(part, mask):
    count = lax.axis_size(AXES[0]) * lax.axis_size(AXES[1])
    return lax.ppermute(part, AXES, [(i, i ^ mask) for i in range(count)])


def sum_rounds():
    count = lax.axis_size(AXES[0]) * lax.axis_size(AXES[1])
    rounds, bit = [], 2
    while bit < count:
        rounds.append([bit, 2 * bit, 3 * bit] if 2 * bit < count else [bit])
        bit *= 4
    return rounds


def sum_round(part, masks):
    others = [exchange(part, mask) for mask in masks]
    if len(others) == 1:
        return part + others[0]
    return (part + others[0]) + (others[1] + others[2])


def sum_all(part):
    part = part + exchange(part, 1)
    for masks in sum_rounds():
        part = sum_round(part, masks)
    return part


def sum_all_halved(part):
    half_rows = part.shape[0] // 2
    first = lax.axis_index(AXES[1]) % 2 == 0
    top, low = part[:half_rows], part[half_rows:]
    kept = jnp.where(first, top, low) + exchange(jnp.where(first, low, top), 1)
    for masks in sum_rounds():
        kept = sum_round(kept, masks)
    other = exchange(kept, 1)
    return jnp.concatenate([jnp.where(first, kept, other), jnp.where(first, other, kept)], axis=0)


def exchange_rows(snapshots):
    name = AXES[0]
    count = lax.axis_size(name)
    if count > 8 or count & (count - 1) or snapshots.shape[0] % 8 or snapshots.shape[1] % (count * LANES):
        return [lax.all_to_all(snapshots, name, split_axis=1, concat_axis=0, tiled=True)]
    blocks = list(deal(snapshots, name))
    for mask in range(1, count):
        blocks[mask] = lax.ppermute(blocks[mask], name, [(i, i ^ mask) for i in range(count)])
    return blocks


def local(snapshots, old_basis, sing_values):
    basis_top, basis_low = basis_pieces(old_basis)
    blocks = exchange_rows(snapshots)
    cell_count = old_basis.shape[0] * lax.axis_size("tile") * lax.axis_size("slab")
    weight_cell = 1.0 / cell_count
    part, snap_rows = local_coeffs(blocks, basis_top, basis_low, weight_cell)
    coeffs = sum_all_halved(part)
    gram_part = residual_gram(coeffs, snap_rows, basis_top, basis_low, weight_cell)
    squares = (sing_values * sing_values)[None, :]
    gram_res = sum_all(gram_part)
    upper, square = opening(lax.optimization_barrier((coeffs, gram_part))[0], squares)
    return updated_basis(
        coeffs, gram_res, squares, upper, square, snap_rows, basis_top, basis_low
    )


def solution(mesh):
    placed = (P("tile", "slab"), P(("slab", "tile"), None), P())
    return jax.shard_map(
        local, mesh=mesh, in_specs=placed, out_specs=P(("slab", "tile"), None), check_vma=False
    )
```

```python
import functools

import jax
import jax.numpy as jnp
from jax import lax
from jax.experimental import pallas as pl
from jax.experimental.pallas import tpu as pltpu
from jax.sharding import PartitionSpec as P

HIGHEST = lax.Precision.HIGHEST
BLOCK = 128
LANES = 128
VMEM = 28 * 1024 * 1024


def dot(left, right, contract=((1,), (0,)), precision=HIGHEST):
    return lax.dot_general(
        left, right, (contract, ((), ())), precision=precision, preferred_element_type=jnp.float32
    )


def spread(value, row):
    return jnp.broadcast_to(value[row : row + 1, :], value.shape)


def lane_spread(value, lane):
    return jnp.broadcast_to(value[:, lane : lane + 1], value.shape)


def total(terms):
    while len(terms) > 1:
        terms = [a + b for a, b in zip(terms[::2], terms[1::2])] + terms[len(terms) // 2 * 2 :]
    return terms[0]


def factor_block(work):
    size = work.shape[0]
    lanes = lax.broadcasted_iota(jnp.int32, (8, size), 1)
    subs = lax.broadcasted_iota(jnp.int32, (8, size), 0)
    first = work[pl.ds(0, 8), :]
    cols = [lane_spread(first, j) for j in range(8)]
    for step in range(size // 8):
        base = 8 * step
        inside = (lanes >= base) & (lanes < base + 8)
        last = step + 1 == size // 8
        below = {
            other: work[pl.ds(8 * other, 8), :] for other in range(step + 1, size // 8)
        }
        beside = {
            other: [lane_spread(rows, base + j) for j in range(8)] for other, rows in below.items()
        }
        ratio, recip = {}, []
        for j in range(8):
            pivot = spread(cols[j], j)
            pivots = pivot if j == 0 else jnp.where(subs == j, pivot, pivots)
            recip.append(1.0 / pivot)
            for k in range(j + 1, 8):
                ratio[j, k] = spread(cols[j], k) * recip[j]
                cols[k] = cols[k] - cols[j] * ratio[j, k]
        if not last:
            near = list(beside[step + 1])
            for j in range(8):
                for k in range(j + 1, 8):
                    near[k] = near[k] - near[j] * ratio[j, k]
            own = [lane_spread(below[step + 1], base + 8 + i) for i in range(8)]
            shares = [near[j] * recip[j] for j in range(8)]
            own = [
                own[i] - total([near[j] * spread(shares[j], i) for j in range(8)]) for i in range(8)
            ]
        row = work[pl.ds(base, 8), :]
        row = jnp.where(inside, jnp.where(lanes - base == subs, 1.0, 0.0), row)
        solved = []
        for j in range(8):
            solved.append(spread(row, j) * recip[j])
            if j < 7:
                row = row - jnp.where(subs > j, cols[j], 0.0) * solved[j]
        work[pl.ds(base, 8), :] = row * lax.rsqrt(pivots)
        for j in reversed(range(7)):
            solved[j] = solved[j] - total([ratio[j, k] * solved[k] for k in range(j + 1, 8)])
        for other, rows in below.items():
            work[pl.ds(8 * other, 8), :] = jnp.where(inside, 0.0, rows) - total(
                [beside[other][j] * solved[j] for j in range(8)]
            )
        if not last:
            cols = own


def tril(value):
    rows = lax.broadcasted_iota(jnp.int32, value.shape, 0)
    return jnp.where(lax.broadcasted_iota(jnp.int32, value.shape, 1) <= rows, value, 0.0)


def split(value, parts):
    pieces = []
    for _ in range(parts):
        pieces.append(value.astype(jnp.bfloat16))
        value = value - pieces[-1].astype(jnp.float32)
    return pieces


def block_dot(left, right):
    a, b, c = split(left, 3)
    d, e, f = split(right, 3)
    both = jnp.concatenate([d, e], axis=0)
    value = dot(jnp.concatenate([a, c], axis=1), jnp.concatenate([f, d], axis=0), precision=None)
    value = value + dot(jnp.concatenate([b, b], axis=1), both, precision=None)
    return value + dot(jnp.concatenate([a, a], axis=1), both, precision=None)


def factor_inverse(gram, work):
    size = gram.shape[0]
    count = size // BLOCK

    def step(index, carry):
        start = pl.multiple_of(index * BLOCK, BLOCK)
        here = pl.ds(start, BLOCK)
        work[...] = gram[here, here]
        factor_block(work)
        inverse = tril(work[...])
        gram[here, here] = jnp.eye(BLOCK, dtype=jnp.float32)
        for block in range(count):

            @pl.when(index == block)
            def _():
                low = BLOCK * block
                high = low + BLOCK
                row = block_dot(inverse, gram[low:high, :])
                gram[low:high, :] = row
                if high < size:
                    gram[high:, low:high] = jnp.zeros((size - high, BLOCK), jnp.float32)
                    gram[high:, :] = gram[high:, :] - block_dot(row[:, high:].T, row)

        return carry

    lax.fori_loop(0, count, step, 0)
    gram[...] = tril(gram[...])


def diagonal(value):
    rows = lax.broadcasted_iota(jnp.int32, value.shape, 0)
    cols = lax.broadcasted_iota(jnp.int32, value.shape, 1)
    return rows == cols


def half(value, offset=0):
    rows = lax.broadcasted_iota(jnp.int32, value.shape, 0) + offset
    cols = lax.broadcasted_iota(jnp.int32, value.shape, 1)
    return jnp.where(rows > cols, value, jnp.where(rows == cols, 0.5 * value, 0.0))


def dot3(left, right, contract=((1,), (0,))):
    left_top, left_low = split(left, 2)
    right_top, right_low = split(right, 2)
    small = dot(left_low, right_top, contract, None) + dot(left_top, right_low, contract, None)
    return dot(left_top, right_top, contract, None) + small


def outer(left, right, exact=True):
    a, b, c = split(left, 3)
    d, e, f = split(right, 3)
    lefts, rights = ([a, a, b, a, c, b], [d, e, d, f, d, e]) if exact else ([a, a, b], [d, e, d])
    left = jnp.concatenate(lefts, axis=0).astype(jnp.float32)
    return dot(left.T.astype(jnp.bfloat16), jnp.concatenate(rights, axis=0), precision=None)


NT = ((1,), (1,))
STOP = 1e-5
NEAR = 0.2
BOUND = 1e30
SHIFT = 4e-6


def step_inverse(low, inverse):
    mid = low.shape[0] // 2
    inverse_top, inverse_low = inverse[:mid, :mid], inverse[...]
    inverse[:mid, :mid] = inverse_top - dot3(low[:mid, :mid], inverse_top)
    inverse[mid:, :] = inverse_low[mid:] - dot3(low[mid:], inverse_low)


def opening_kernel(coeffs_ref, squares_ref, upper, square):
    coeffs = coeffs_ref[...]
    mid = coeffs.shape[1] // 2
    value = outer(coeffs, coeffs)
    upper[...] = value + jnp.where(diagonal(value), squares_ref[...], 0.0)
    square[:mid, :] = dot(upper[:mid, :], upper[...])
    square[mid:, :mid] = jnp.zeros((mid, mid), jnp.float32)
    square[mid:, mid:] = dot(upper[mid:, :], upper[:, mid:])


def opening(coeffs, squares):
    modes = coeffs.shape[1]
    spec = pl.BlockSpec(memory_space=pltpu.VMEM)
    shape = jax.ShapeDtypeStruct((modes, modes), jnp.float32)
    return pl.pallas_call(
        opening_kernel, out_shape=(shape, shape), in_specs=[spec] * 2, out_specs=(spec, spec),
        compiler_params=pltpu.CompilerParams(vmem_limit_bytes=VMEM),
        cost_estimate=pl.CostEstimate(
            flops=12 * modes**3, bytes_accessed=8 * modes**2, transcendentals=0
        ),
    )(coeffs, squares)


def pieces_kernel(basis_ref, top, low):
    rows = basis_ref.shape[0]
    chunk = chunk_of(rows)
    for start in range(0, rows, chunk):
        here = pl.ds(start, chunk)
        top[here, :], low[here, :] = split(basis_ref[here, :], 2)


def basis_pieces(old_basis):
    rows, modes = old_basis.shape
    spec = pl.BlockSpec(memory_space=pltpu.VMEM)
    shape = jax.ShapeDtypeStruct((rows, modes), jnp.bfloat16)
    return pl.pallas_call(
        pieces_kernel, out_shape=(shape, shape), in_specs=[spec], out_specs=(spec, spec),
        compiler_params=pltpu.CompilerParams(vmem_limit_bytes=VMEM),
        cost_estimate=pl.CostEstimate(
            flops=1000 * rows * modes, bytes_accessed=8 * rows * modes, transcendentals=0
        ),
    )(old_basis)


def deal_kernel(name, snaps_ref, *blocks):
    cells = blocks[0].shape[1]
    index = lax.axis_index(name)
    for mask, block in enumerate(blocks):
        start = pl.multiple_of(jnp.bitwise_xor(index, mask) * cells, LANES)
        block[...] = snaps_ref[:, pl.ds(start, cells)]


def deal(snapshots, name):
    count = lax.axis_size(name)
    rows, cells = snapshots.shape[0], snapshots.shape[1] // count
    spec = pl.BlockSpec(memory_space=pltpu.VMEM)
    return pl.pallas_call(
        functools.partial(deal_kernel, name),
        out_shape=[jax.ShapeDtypeStruct((rows, cells), jnp.float32)] * count,
        in_specs=[spec], out_specs=[spec] * count,
        compiler_params=pltpu.CompilerParams(vmem_limit_bytes=VMEM),
    )(snapshots)


def coeffs_kernel(name, weight, count, *refs):
    top_ref, low_ref, out_ref, snaps_ref = refs[count:]
    if count == 1:
        snaps_ref[...] = refs[0][...]
    else:
        rows = refs[0].shape[0]
        index = lax.axis_index(name)
        for mask in range(count):
            start = pl.multiple_of(jnp.bitwise_xor(index, mask) * rows, rows)
            snaps_ref[pl.ds(start, rows), :] = refs[mask][...]
    snaps = snaps_ref.shape[0]
    top, low = split(snaps_ref[...], 2)
    value = dot(jnp.concatenate([top, low], axis=0), top_ref[...], precision=None)
    value = value[:snaps] + (value[snaps:] + dot(top, low_ref[...], precision=None))
    out_ref[...] = value * weight


def local_coeffs(blocks, basis_top, basis_low, weight):
    count = len(blocks)
    rows, modes = basis_top.shape
    snaps = count * blocks[0].shape[0]
    spec = pl.BlockSpec(memory_space=pltpu.VMEM)
    return pl.pallas_call(
        functools.partial(coeffs_kernel, AXES[0], weight, count),
        out_shape=(
            jax.ShapeDtypeStruct((snaps, modes), jnp.float32),
            jax.ShapeDtypeStruct((snaps, rows), jnp.float32),
        ),
        in_specs=[spec] * (count + 2), out_specs=(spec, spec),
        compiler_params=pltpu.CompilerParams(vmem_limit_bytes=VMEM),
    )(*blocks, basis_top, basis_low)


def residual_kernel(weight, coeffs_ref, snaps_ref, top_ref, low_ref, out_ref):
    snaps = snaps_ref.shape[0]
    top, low = split(coeffs_ref[...], 2)
    value = dot(jnp.concatenate([top, low], axis=0), top_ref[...], NT, None)
    value = value[:snaps] + (value[snaps:] + dot(top, low_ref[...], NT, None))
    top, low = split(snaps_ref[...] - value, 2)
    value = dot(jnp.concatenate([top, low], axis=0), top, NT, None)
    out_ref[...] = (value[:snaps] + (value[snaps:] + value[snaps:].T)) * weight


def residual_gram(coeffs, snap_rows, basis_top, basis_low, weight):
    snaps = coeffs.shape[0]
    spec = pl.BlockSpec(memory_space=pltpu.VMEM)
    return pl.pallas_call(
        functools.partial(residual_kernel, weight),
        out_shape=jax.ShapeDtypeStruct((snaps, snaps), jnp.float32),
        in_specs=[spec] * 4, out_specs=spec,
        compiler_params=pltpu.CompilerParams(vmem_limit_bytes=VMEM),
    )(coeffs, snap_rows, basis_top, basis_low)


def rotation(coeffs_ref, gram_ref, upper, square_ref, inverse, second, work):
    coeffs = coeffs_ref[...]
    mid = coeffs.shape[1] // 2

    def first_gram():
        second[...] = square_ref[...] + outer(coeffs, dot(gram_ref[...], coeffs))

    first_gram()

    def far(carry):
        return jnp.logical_not(carry[1] < NEAR) & (carry[0] < 12)

    one = jnp.where(diagonal(square_ref), 1.0, 0.0)

    def mirror():
        second[:mid, mid:] = second[mid:, :mid].T

    def factor_pass(carry):
        count, _, fresh, shift = carry

        @pl.when(count > 0)
        def _():
            second[...] = second[...] + one

        factor_inverse(second, work)

        @pl.when(fresh == 1)
        def _():
            inverse[...] = second[...]

        @pl.when(fresh == 0)
        def _():
            inverse[...] = dot(second[...], inverse[...])

        part = dot3(coeffs, inverse[...], NT)
        side = dot3(gram_ref[...], part)
        extra = outer(side, part, False) - one
        second[:mid, :] = dot(inverse[:mid, :mid], upper[:mid, :])
        second[mid:, :] = dot(inverse[mid:, :], upper[...])
        stacked = second[...]
        rest_low = dot3(stacked[mid:], stacked, NT) + extra[mid:]
        rest_top = dot3(stacked[:mid], stacked[:mid], NT) + extra[:mid, :mid]
        second[:mid, :mid] = rest_top
        second[mid:, :] = rest_low
        size = (
            jnp.sum(rest_top * rest_top)
            + jnp.sum(rest_low[:, mid:] * rest_low[:, mid:])
            + 2.0 * jnp.sum(rest_low[:, :mid] * rest_low[:, :mid])
        )
        failed = jnp.logical_not(size < BOUND)

        @pl.when(failed)
        def _():
            first_gram()
            ends = one * second[...]
            second[...] = second[...] + (shift * jnp.max(ends) - 1.0) * one

        @pl.when(jnp.logical_not(failed) & (size >= STOP))
        def _():
            mirror()

        return count + 1, size, failed.astype(jnp.int32), jnp.where(failed, 8.0 * shift, shift)

    first = (jnp.int32(0), jnp.float32(BOUND), jnp.int32(1), jnp.float32(SHIFT))
    size = lax.while_loop(far, factor_pass, first)[1]

    def more(carry):
        return (carry[0] >= STOP) & (carry[1] < 16)

    def newton(carry):
        rest = second[...]
        low = half(rest)
        step_inverse(low, inverse)
        mixed = dot3(low, rest)
        rest = dot3(low + mixed, low, NT) - mixed - mixed.T
        second[...] = rest
        return jnp.sum(rest * rest), carry[1] + 1

    lax.while_loop(more, newton, (size, jnp.int32(0)))
    step_inverse(half(second[...]), inverse)


def update_kernel(
    coeffs_ref, gram_ref, squares_ref, upper, square_ref, snaps_ref, top_ref, low_ref, out_hbm,
    inverse, second, work, out, stored,
):
    rows, modes = top_ref.shape
    mid = modes // 2
    rotation(coeffs_ref, gram_ref, upper, square_ref, inverse, second, work)
    final = inverse[...]
    turn_top, turn_low = split(final * squares_ref[...], 2)
    across_top, across_low = split(dot(coeffs_ref[...], final, NT), 2)
    across = jnp.concatenate([across_top, across_low, across_top], axis=0)
    chunk = chunk_of(rows)
    copies = []
    for start in range(0, rows, chunk):
        here = pl.ds(start, chunk)
        snaps_top, snaps_low = split(snaps_ref[:, pl.ds(start, chunk)], 2)
        mixed = jnp.concatenate([snaps_top, snaps_top, snaps_low], axis=0).astype(jnp.float32)
        base = dot(mixed.T.astype(jnp.bfloat16), across, precision=None)
        top, low = top_ref[here, :], low_ref[here, :]
        for cols, depth in ((slice(0, mid), mid), (slice(mid, modes), modes)):
            value = base[:, cols]
            for a, b in ((low, turn_top), (top, turn_low), (top, turn_top)):
                value = value + dot(a[:, :depth], b[cols, :depth], NT, None)
            out[here, cols] = value.astype(out.dtype)
        copies.append(pltpu.make_async_copy(out.at[here, :], out_hbm.at[here, :], stored.at[start // chunk]))
        copies[-1].start()
    for copy in copies:
        copy.wait()


def chunk_of(rows):
    for chunk in (640, 512, 384, 256, 128):
        if rows % chunk == 0:
            return chunk
    return rows


def updated_basis(coeffs, gram_res, squares, upper, square, snap_rows, basis_top, basis_low):
    rows, modes = basis_top.shape
    whole = pltpu.VMEM((modes, modes), jnp.float32)
    spec = pl.BlockSpec(memory_space=pltpu.VMEM)
    far = pl.BlockSpec(memory_space=pl.ANY)
    return pl.pallas_call(
        update_kernel,
        out_shape=jax.ShapeDtypeStruct((rows, modes), jnp.bfloat16),
        in_specs=[spec] * 8,
        out_specs=far,
        scratch_shapes=[
            whole, whole, pltpu.VMEM((BLOCK, BLOCK), jnp.float32),
            pltpu.VMEM((rows, modes), jnp.bfloat16), pltpu.SemaphoreType.DMA((rows // chunk_of(rows),)),
        ],
        compiler_params=pltpu.CompilerParams(vmem_limit_bytes=VMEM),
    )(coeffs, gram_res, squares, upper, square, snap_rows, basis_top, basis_low)


AXES = ("tile", "slab")


def exchange(part, mask):
    count = lax.axis_size(AXES[0]) * lax.axis_size(AXES[1])
    return lax.ppermute(part, AXES, [(i, i ^ mask) for i in range(count)])


def sum_rounds():
    count = lax.axis_size(AXES[0]) * lax.axis_size(AXES[1])
    rounds, bit = [], 2
    while bit < count:
        rounds.append([bit, 2 * bit, 3 * bit] if 2 * bit < count else [bit])
        bit *= 4
    return rounds


def sum_round(part, masks):
    others = [exchange(part, mask) for mask in masks]
    if len(others) == 1:
        return part + others[0]
    return (part + others[0]) + (others[1] + others[2])


def sum_all(part):
    part = part + exchange(part, 1)
    for masks in sum_rounds():
        part = sum_round(part, masks)
    return part


def sum_all_halved(part):
    half_rows = part.shape[0] // 2
    first = lax.axis_index(AXES[1]) % 2 == 0
    top, low = part[:half_rows], part[half_rows:]
    kept = jnp.where(first, top, low) + exchange(jnp.where(first, low, top), 1)
    for masks in sum_rounds():
        kept = sum_round(kept, masks)
    other = exchange(kept, 1)
    return jnp.concatenate([jnp.where(first, kept, other), jnp.where(first, other, kept)], axis=0)


def exchange_rows(snapshots):
    name = AXES[0]
    count = lax.axis_size(name)
    if count > 8 or count & (count - 1) or snapshots.shape[0] % 8 or snapshots.shape[1] % (count * LANES):
        return [lax.all_to_all(snapshots, name, split_axis=1, concat_axis=0, tiled=True)]
    blocks = list(deal(snapshots, name))
    for mask in range(1, count):
        blocks[mask] = lax.ppermute(blocks[mask], name, [(i, i ^ mask) for i in range(count)])
    return blocks


def local(snapshots, old_basis, sing_values):
    basis_top, basis_low = basis_pieces(old_basis)
    blocks = exchange_rows(snapshots)
    cell_count = old_basis.shape[0] * lax.axis_size("tile") * lax.axis_size("slab")
    weight_cell = 1.0 / cell_count
    part, snap_rows = local_coeffs(blocks, basis_top, basis_low, weight_cell)
    coeffs = sum_all_halved(part)
    gram_part = residual_gram(coeffs, snap_rows, basis_top, basis_low, weight_cell)
    squares = (sing_values * sing_values)[None, :]
    gram_res = sum_all(gram_part)
    upper, square = opening(lax.optimization_barrier((coeffs, gram_part))[0], squares)
    return updated_basis(
        coeffs, gram_res, squares, upper, square, snap_rows, basis_top, basis_low
    )


def solution(mesh):
    placed = (P("tile", "slab"), P(("slab", "tile"), None), P())
    return jax.shard_map(
        local, mesh=mesh, in_specs=placed, out_specs=P(("slab", "tile"), None), check_vma=False
    )
```
